32 devices in a mesh: data: 4 (over y, z), tp: 8 (over x, core).
Axes of the slice: x: 4, y: 2, z: 2, core: 2. Of those that a mesh axis runs over, the one named last changes fastest.
The devices are a block of a 4x4x8 slice.
Arguments:
- attn_out: bfloat16 [1024, 16384], P('data', 'tp'), parts along dimension 0
- w_out: bfloat16 [16384, 16384], P('tp')
- residual: bfloat16 [1024, 16384], P('data', 'tp'), parts along dimension 0
- norm_gain: float32 [16384], P('tp')
Outputs:
- output 1: bfloat16 [1024, 16384], P('data', 'tp'), parts along dimension 0
- output 2: bfloat16 [1024, 16384], P('data', 'tp'), parts along dimension 0
There are 4 independent parts. The reference program is written for one: setup_inputs(seed, part) draws one part's arguments, and reference() takes and returns one part's arrays. A program takes and returns all parts, laid end to end along the dimension named above; an argument that names none is the same for every part.
All inputs are finite; a program needn't handle non-finite values.
Results may differ from the reference program's by a relative error of at most 0.00634236.
Values are sent between devices in bfloat16 or wider.
A program may use at most 768 MiB of HBM per device.

```python
import jax
import jax.numpy as jnp
from jax import lax

D_MODEL = 16384
N_HEADS = 128
HEAD_DIM = 128
TOKENS = 256
EPS = 1e-5


def setup_inputs(seed: int = 0, part: int = 0) -> dict:
    proj_width = N_HEADS * HEAD_DIM
    part_key = jax.random.fold_in(jax.random.key(seed), part)
    key_attn, key_resid = jax.random.split(part_key, 2)
    key_weight, key_gain = jax.random.split(jax.random.key(seed + 1), 2)
    attn_out = jax.random.normal(key_attn, (TOKENS, proj_width), jnp.float32).astype(jnp.bfloat16)
    weight_vals = jax.random.normal(key_weight, (proj_width, D_MODEL), jnp.float32) * proj_width ** -0.5
    w_out = weight_vals.astype(jnp.bfloat16)
    residual = jax.random.normal(key_resid, (TOKENS, D_MODEL), jnp.float32).astype(jnp.bfloat16)
    norm_gain = jax.random.uniform(key_gain, (D_MODEL,), jnp.float32, 0.5, 1.5)
    return {"attn_out": attn_out, "w_out": w_out, "residual": residual, "norm_gain": norm_gain}


def reference(attn_out, w_out, residual, norm_gain):
    projected = jnp.dot(attn_out, w_out, preferred_element_type=jnp.float32)
    hidden = residual.astype(jnp.float32) + projected
    mean_sq = jnp.mean(hidden * hidden, axis=-1, keepdims=True)
    normed = hidden * lax.rsqrt(mean_sq + EPS) * norm_gain
    return (hidden.astype(jnp.bfloat16), normed.astype(jnp.bfloat16))
```

```python
import functools

import jax
import jax.numpy as jnp
from jax import lax
from jax.experimental import pallas as pl
from jax.experimental.pallas import tpu as pltpu
from jax.sharding import PartitionSpec as P

EPS = 1e-5
CORES = 2
COLS = 512
W_SLOTS = 3


def kernel(
    tp, tok_rows, d_local, a_hbm, w_hbm, r_hbm, g_ref, hid_hbm, nrm_hbm,
    a, w, part, recv, relay_out, relay_in, res, hid, hid_bf, nrm_bf, sq_lanes, sq_all,
    a_sem, w_sem, r_sem, send_sem, recv_sem, rsend_sem, rrecv_sem, qsend_sem, qrecv_sem,
    out_sem,
):
    chips = tp // CORES
    half = d_local // 2
    pp = half // COLS
    blk = 4 * pp
    me = lax.axis_index("tp")
    chip, core = me // CORES, me % CORES

    def w_col(g):
        b, i = g % 2, (g % blk) // 2
        s, p, ph = i % 2, i // 2, g // blk
        is0 = (3 - ph) * (2 - ph) * (1 - ph) // 6
        is1 = ph * (3 - ph) * (2 - ph) // 2
        is2 = ph * (3 - ph) * (ph - 1) // 2
        kept = ph // 2
        step = 2 * s - 1
        hop = is0 * 2 + is1 * step + kept * (1 - b) * step
        to_core = (1 - kept) * b + is2 * (1 - core) + (kept - is2) * core
        in_half = s + is1 * (1 - 2 * s)
        to = ((chip + chips + hop) % chips) * CORES + to_core
        return to * d_local + in_half * half + p * COLS

    def w_copy(g):
        slot = g % W_SLOTS
        cols = pl.ds(pl.multiple_of(w_col(g), COLS), COLS)
        return pltpu.make_async_copy(w_hbm.at[:, cols], w.at[slot], w_sem.at[slot])

    def piece_copy(g):
        b, i = g % 2, (g % blk) // 2
        s, ph = i % 2, g // blk
        far = 1 - ph // 2
        to_chip = (chip + chips + far * (2 * s - 1)) % chips
        to_core = far * b + (1 - far) * (1 - core)
        slot = g + far * (core - b)
        return pltpu.make_async_remote_copy(
            src_ref=part.at[g],
            dst_ref=recv.at[slot],
            send_sem=send_sem.at[g],
            recv_sem=recv_sem.at[slot],
            device_id={"tp": to_chip * CORES + to_core},
            device_id_type=pl.DeviceIdType.MESH,
        )

    def recv_wait(slot):
        pltpu.make_async_copy(recv.at[slot], recv.at[slot], recv_sem.at[slot]).wait()

    def relay_copy(i):
        to_chip = (chip + chips + 2 * (i % 2) - 1) % chips
        return pltpu.make_async_remote_copy(
            src_ref=relay_out.at[i],
            dst_ref=relay_in.at[i],
            send_sem=rsend_sem.at[i],
            recv_sem=rrecv_sem.at[i],
            device_id={"tp": to_chip * CORES + core},
            device_id_type=pl.DeviceIdType.MESH,
        )

    def sq_copy(j):
        return pltpu.make_async_remote_copy(
            src_ref=sq_all.at[me],
            dst_ref=sq_all.at[me],
            send_sem=qsend_sem.at[j],
            recv_sem=qrecv_sem.at[me],
            device_id={"tp": (me + j) % tp},
            device_id_type=pl.DeviceIdType.MESH,
        )

    a_copy = pltpu.make_async_copy(a_hbm, a, a_sem)
    r_copy = pltpu.make_async_copy(r_hbm, res, r_sem)
    a_copy.start()
    for g in range(W_SLOTS):
        w_copy(g).start()
    barrier = pltpu.get_barrier_semaphore()
    for j in range(1, tp):
        pl.semaphore_signal(
            barrier, inc=1, device_id={"tp": (me + j) % tp}, device_id_type=pl.DeviceIdType.MESH
        )
    pl.semaphore_wait(barrier, tp - 1)
    a_copy.wait()

    def project(g, carry):
        slot = g % W_SLOTS
        w_copy(g).wait()
        part[g] = jnp.dot(a[...], w[slot], preferred_element_type=jnp.float32).astype(jnp.bfloat16)

        @pl.when(g < 3 * blk)
        def _():
            piece_copy(g).start()

        @pl.when(g + W_SLOTS < 4 * blk)
        def _():
            w_copy(g + W_SLOTS).start()

        return carry

    lax.fori_loop(0, 4 * blk, project, 0)
    r_copy.start()

    def relay(i, carry):
        recv_wait(2 * i)
        recv_wait(2 * i + 1)
        recv_wait(2 * blk + 2 * i)
        relay_out[i] = (
            recv[2 * i].astype(jnp.float32)
            + recv[2 * i + 1].astype(jnp.float32)
            + recv[2 * blk + 2 * i].astype(jnp.float32)
            + part[3 * blk + 2 * i].astype(jnp.float32)
        )
        relay_copy(i).start()
        return carry

    lax.fori_loop(0, 2 * pp, relay, 0)
    r_copy.wait()

    def columns(i):
        return pl.ds(pl.multiple_of((i % 2) * half + (i // 2) * COLS, COLS), COLS)

    def gather(i, carry):
        direct = blk + 2 * (i + 1 - 2 * (i % 2))
        recv_wait(direct)
        recv_wait(direct + 1)
        recv_wait(2 * blk + 2 * i + 1)
        hid[i] = (
            res[:, columns(i)].astype(jnp.float32)
            + part[3 * blk + 2 * i + 1].astype(jnp.float32)
            + recv[2 * blk + 2 * i + 1].astype(jnp.float32)
            + recv[direct].astype(jnp.float32)
            + recv[direct + 1].astype(jnp.float32)
        )
        return carry

    lax.fori_loop(0, 2 * pp, gather, 0)
    sq_lanes[...] = jnp.zeros_like(sq_lanes)

    def hid_out(i):
        return pltpu.make_async_copy(
            hid_bf.at[:, columns(i)], hid_hbm.at[:, columns(i)], out_sem.at[i]
        )

    def nrm_out(i):
        return pltpu.make_async_copy(
            nrm_bf.at[:, columns(i)], nrm_hbm.at[:, columns(i)], out_sem.at[2 * pp + i]
        )

    def finish(i, carry):
        relay_copy(i).wait_recv()
        h = hid[i] + relay_in[i]
        hid[i] = h
        hid_bf[:, columns(i)] = h.astype(jnp.bfloat16)
        hid_out(i).start()
        sq = h * h
        total = sq_lanes[...]
        for c in range(COLS // 128):
            total += sq[:, c * 128 : (c + 1) * 128]
        sq_lanes[...] = total
        return carry

    lax.fori_loop(0, 2 * pp, finish, 0)

    by_lane = jnp.transpose(sq_lanes[...])
    sq_all[me] = jnp.sum(by_lane.reshape(16, 8, tok_rows), axis=0)
    for j in range(1, tp):
        sq_copy(j).start()
    for j in range(1, tp):
        peer = (me + j) % tp
        pltpu.make_async_copy(sq_all.at[peer], sq_all.at[peer], qrecv_sem.at[peer]).wait()
    sq_total = jnp.sum(jnp.sum(sq_all[...], axis=0), axis=0, keepdims=True)
    scale_row = lax.rsqrt(sq_total / (d_local * tp) + EPS)
    scale = jnp.transpose(jnp.broadcast_to(scale_row, (128, tok_rows)))

    def normalize(i, carry):
        for c in range(COLS // 128):
            lanes = pl.ds(pl.multiple_of((i % 2) * half + (i // 2) * COLS + c * 128, 128), 128)
            normed = hid[i, :, c * 128 : (c + 1) * 128] * scale * g_ref[:, lanes]
            nrm_bf[:, lanes] = normed.astype(jnp.bfloat16)
        nrm_out(i).start()
        return carry

    lax.fori_loop(0, 2 * pp, normalize, 0)

    def drain(g, carry):
        piece_copy(g).wait_send()
        return carry

    lax.fori_loop(0, 3 * blk, drain, 0)
    for i in range(2 * pp):
        relay_copy(i).wait_send()
        hid_out(i).wait()
        nrm_out(i).wait()
    for j in range(1, tp):
        sq_copy(j).wait_send()


def solution(mesh):
    tp = mesh.shape["tp"]

    def local_step(attn_blk, w_blk, resid_blk, gain_blk):
        tok_rows, depth = attn_blk.shape
        d_local = resid_blk.shape[1]
        pp = d_local // 2 // COLS
        f32, bf16 = jnp.float32, jnp.bfloat16
        piece = (tok_rows, COLS)
        dma = pltpu.SemaphoreType.DMA
        anywhere = pl.BlockSpec(memory_space=pl.ANY)
        return pl.pallas_call(
            functools.partial(kernel, tp, tok_rows, d_local),
            out_shape=[jax.ShapeDtypeStruct((tok_rows, d_local), bf16)] * 2,
            in_specs=[anywhere] * 3 + [pl.BlockSpec(memory_space=pltpu.VMEM)],
            out_specs=[anywhere] * 2,
            scratch_shapes=[
                pltpu.VMEM((tok_rows, depth), bf16),
                pltpu.VMEM((W_SLOTS, depth, COLS), bf16),
                pltpu.VMEM((16 * pp, *piece), bf16),
                pltpu.VMEM((12 * pp, *piece), bf16),
                pltpu.VMEM((2 * pp, *piece), f32),
                pltpu.VMEM((2 * pp, *piece), f32),
                pltpu.VMEM((tok_rows, d_local), bf16),
                pltpu.VMEM((2 * pp, *piece), f32),
                pltpu.VMEM((tok_rows, d_local), bf16),
                pltpu.VMEM((tok_rows, d_local), bf16),
                pltpu.VMEM((tok_rows, 128), f32),
                pltpu.VMEM((tp, 8, tok_rows), f32),
                dma,
                dma((W_SLOTS,)),
                dma,
                dma((12 * pp,)),
                dma((12 * pp,)),
                dma((2 * pp,)),
                dma((2 * pp,)),
                dma((tp,)),
                dma((tp,)),
                dma((4 * pp,)),
            ],
            compiler_params=pltpu.CompilerParams(
                collective_id=0, has_side_effects=True, vmem_limit_bytes=60 * 2**20
            ),
            name="project_reduce_norm",
        )(attn_blk, w_blk, resid_blk, gain_blk.reshape(1, d_local))

    return jax.shard_map(
        local_step,
        mesh=mesh,
        in_specs=(P("data", "tp"), P("tp", None), P("data", "tp"), P("tp")),
        out_specs=(P("data", "tp"), P("data", "tp")),
        check_vma=False,
    )
```

```python
import functools

import jax
import jax.numpy as jnp
from jax import lax
from jax.experimental import pallas as pl
from jax.experimental.pallas import tpu as pltpu
from jax.sharding import PartitionSpec as P

EPS = 1e-5
CORES = 2
COLS = 512
W_SLOTS = 3
ROWS = 128


def kernel(
    tp, tok_rows, d_local, a_hbm, w_hbm, r_hbm, g_ref, hid_out, nrm_out,
    a, w, part, recv, relay_out, relay_in, res, hid, sq_all,
    a_sem, w_sem, r_sem, send_sem, recv_sem, rsend_sem, rrecv_sem, qsend_sem, qrecv_sem,
):
    chips = tp // CORES
    half = d_local // 2
    pp = half // COLS
    blk = 4 * pp
    me = lax.axis_index("tp")
    chip, core = me // CORES, me % CORES

    def w_col(g):
        b, i = g % 2, (g % blk) // 2
        s, p, ph = i % 2, i // 2, g // blk
        is0 = (3 - ph) * (2 - ph) * (1 - ph) // 6
        is1 = ph * (3 - ph) * (2 - ph) // 2
        is2 = ph * (3 - ph) * (ph - 1) // 2
        kept = ph // 2
        step = 2 * s - 1
        hop = is0 * 2 + is1 * step + kept * (1 - b) * step
        to_core = (1 - kept) * b + is2 * (1 - core) + (kept - is2) * core
        in_half = s + is1 * (1 - 2 * s)
        to = ((chip + chips + hop) % chips) * CORES + to_core
        return to * d_local + in_half * half + p * COLS

    def w_copy(g):
        slot = g % W_SLOTS
        cols = pl.ds(pl.multiple_of(w_col(g), COLS), COLS)
        return pltpu.make_async_copy(w_hbm.at[:, cols], w.at[slot], w_sem.at[slot])

    def piece_copy(g):
        b, i = g % 2, (g % blk) // 2
        s, ph = i % 2, g // blk
        far = 1 - ph // 2
        to_chip = (chip + chips + far * (2 * s - 1)) % chips
        to_core = far * b + (1 - far) * (1 - core)
        slot = g + far * (core - b)
        return pltpu.make_async_remote_copy(
            src_ref=part.at[g],
            dst_ref=recv.at[slot],
            send_sem=send_sem.at[g],
            recv_sem=recv_sem.at[slot],
            device_id={"tp": to_chip * CORES + to_core},
            device_id_type=pl.DeviceIdType.MESH,
        )

    def recv_wait(slot):
        pltpu.make_async_copy(recv.at[slot], recv.at[slot], recv_sem.at[slot]).wait()

    def relay_copy(i):
        to_chip = (chip + chips + 2 * (i % 2) - 1) % chips
        return pltpu.make_async_remote_copy(
            src_ref=relay_out.at[i],
            dst_ref=relay_in.at[i],
            send_sem=rsend_sem.at[i],
            recv_sem=rrecv_sem.at[i],
            device_id={"tp": to_chip * CORES + core},
            device_id_type=pl.DeviceIdType.MESH,
        )

    def sq_copy(rb, j):
        return pltpu.make_async_remote_copy(
            src_ref=sq_all.at[rb, me],
            dst_ref=sq_all.at[rb, me],
            send_sem=qsend_sem.at[rb, j],
            recv_sem=qrecv_sem.at[rb, me],
            device_id={"tp": (me + j) % tp},
            device_id_type=pl.DeviceIdType.MESH,
        )

    a_copy = pltpu.make_async_copy(a_hbm, a, a_sem)
    r_copy = pltpu.make_async_copy(r_hbm, res, r_sem)
    a_copy.start()
    for g in range(W_SLOTS):
        w_copy(g).start()
    barrier = pltpu.get_barrier_semaphore()
    for j in range(1, tp):
        pl.semaphore_signal(
            barrier, inc=1, device_id={"tp": (me + j) % tp}, device_id_type=pl.DeviceIdType.MESH
        )
    pl.semaphore_wait(barrier, tp - 1)
    a_copy.wait()

    def project(g, carry):
        slot = g % W_SLOTS
        w_copy(g).wait()
        part[g] = jnp.dot(a[...], w[slot], preferred_element_type=jnp.float32).astype(jnp.bfloat16)

        @pl.when(g < 3 * blk)
        def _():
            piece_copy(g).start()

        @pl.when(g + W_SLOTS < 4 * blk)
        def _():
            w_copy(g + W_SLOTS).start()

        return carry

    lax.fori_loop(0, 4 * blk, project, 0)
    r_copy.start()

    def row_block(rb):
        return pl.ds(pl.multiple_of(rb * ROWS, ROWS), ROWS)

    for i in range(2 * pp):
        recv_wait(2 * i)
        recv_wait(2 * i + 1)
        recv_wait(2 * blk + 2 * i)

    def relay(j, carry):
        rows, s = row_block(j // 2), j % 2
        for p in range(pp):
            i = 2 * p + s
            relay_out[j, :, p * COLS : (p + 1) * COLS] = (
                recv[2 * i, rows].astype(jnp.float32)
                + recv[2 * i + 1, rows].astype(jnp.float32)
                + recv[2 * blk + 2 * i, rows].astype(jnp.float32)
                + part[3 * blk + 2 * i, rows].astype(jnp.float32)
            )
        relay_copy(j).start()
        return carry

    lax.fori_loop(0, 2 * (tok_rows // ROWS), relay, 0)
    r_copy.wait()

    def gather(i, carry):
        cols = pl.ds(pl.multiple_of((i % 2) * half + (i // 2) * COLS, COLS), COLS)
        direct = blk + 2 * (i + 1 - 2 * (i % 2))
        recv_wait(direct)
        recv_wait(direct + 1)
        recv_wait(2 * blk + 2 * i + 1)
        hid[:, cols] = (
            res[:, cols].astype(jnp.float32)
            + part[3 * blk + 2 * i + 1].astype(jnp.float32)
            + recv[2 * blk + 2 * i + 1].astype(jnp.float32)
            + recv[direct].astype(jnp.float32)
            + recv[direct + 1].astype(jnp.float32)
        )
        return carry

    lax.fori_loop(0, 2 * pp, gather, 0)

    def finish(rb, carry):
        rows = row_block(rb)
        total = jnp.zeros((ROWS, 128), jnp.float32)
        for s in range(2):
            relay_copy(2 * rb + s).wait_recv()
            for c in range(0, half, 128):
                cols = slice(s * half + c, s * half + c + 128)
                h = hid[rows, cols] + relay_in[2 * rb + s, :, c : c + 128]
                hid[rows, cols] = h
                hid_out[rows, cols] = h.astype(jnp.bfloat16)
                total += h * h
        sq_all[rb, me] = jnp.sum(jnp.transpose(total).reshape(16, 8, ROWS), axis=0)
        for j in range(1, tp):
            sq_copy(rb, j).start()
        for j in range(1, tp):
            peer = (me + j) % tp
            pltpu.make_async_copy(
                sq_all.at[rb, peer], sq_all.at[rb, peer], qrecv_sem.at[rb, peer]
            ).wait()
        sq_total = jnp.sum(jnp.sum(sq_all[rb], axis=0), axis=0, keepdims=True)
        scale_row = lax.rsqrt(sq_total / (d_local * tp) + EPS)
        scale = jnp.transpose(jnp.broadcast_to(scale_row, (128, ROWS)))
        for c in range(0, d_local, 128):
            normed = hid[rows, c : c + 128] * scale * g_ref[:, c : c + 128]
            nrm_out[rows, c : c + 128] = normed.astype(jnp.bfloat16)
        return carry

    lax.fori_loop(0, tok_rows // ROWS, finish, 0)

    def drain(g, carry):
        piece_copy(g).wait_send()
        return carry

    lax.fori_loop(0, 3 * blk, drain, 0)
    for j in range(2 * (tok_rows // ROWS)):
        relay_copy(j).wait_send()
    for rb in range(tok_rows // ROWS):
        for j in range(1, tp):
            sq_copy(rb, j).wait_send()


def solution(mesh):
    tp = mesh.shape["tp"]

    def local_step(attn_blk, w_blk, resid_blk, gain_blk):
        tok_rows, depth = attn_blk.shape
        d_local = resid_blk.shape[1]
        pp = d_local // 2 // COLS
        blocks = tok_rows // ROWS
        f32, bf16 = jnp.float32, jnp.bfloat16
        piece = (tok_rows, COLS)
        dma = pltpu.SemaphoreType.DMA
        anywhere = pl.BlockSpec(memory_space=pl.ANY)
        return pl.pallas_call(
            functools.partial(kernel, tp, tok_rows, d_local),
            out_shape=[pltpu.VMEM((tok_rows, d_local), bf16)] * 2,
            in_specs=[anywhere] * 3 + [pl.BlockSpec(memory_space=pltpu.VMEM)],
            out_specs=[pl.BlockSpec(memory_space=pltpu.VMEM)] * 2,
            scratch_shapes=[
                pltpu.VMEM((tok_rows, depth), bf16),
                pltpu.VMEM((W_SLOTS, depth, COLS), bf16),
                pltpu.VMEM((16 * pp, *piece), bf16),
                pltpu.VMEM((12 * pp, *piece), bf16),
                pltpu.VMEM((2 * blocks, ROWS, d_local // 2), f32),
                pltpu.VMEM((2 * blocks, ROWS, d_local // 2), f32),
                pltpu.VMEM((tok_rows, d_local), bf16),
                pltpu.VMEM((tok_rows, d_local), f32),
                pltpu.VMEM((blocks, tp, 8, ROWS), f32),
                dma,
                dma((W_SLOTS,)),
                dma,
                dma((12 * pp,)),
                dma((12 * pp,)),
                dma((2 * blocks,)),
                dma((2 * blocks,)),
                dma((blocks, tp)),
                dma((blocks, tp)),
            ],
            compiler_params=pltpu.CompilerParams(
                collective_id=0, has_side_effects=True, vmem_limit_bytes=56 * 2**20
            ),
            name="project_reduce_norm",
        )(attn_blk, w_blk, resid_blk, gain_blk.reshape(1, d_local))

    return jax.shard_map(
        local_step,
        mesh=mesh,
        in_specs=(P("data", "tp"), P("tp", None), P("data", "tp"), P("tp")),
        out_specs=(P("data", "tp"), P("data", "tp")),
        check_vma=False,
    )
```

```python
import functools

import jax
import jax.numpy as jnp
from jax import lax
from jax.experimental import pallas as pl
from jax.experimental.pallas import tpu as pltpu
from jax.sharding import PartitionSpec as P

EPS = 1e-5
CORES = 2
COLS = 256
W_SLOTS = 6
ROWS = 128
OUT_ROWS = 64


def reduce_kernel(
    tp, d_local, a_hbm, w_hbm, r_hbm, g_hbm, hid, hid_bf, sq_sum, gain,
    a, w, part, recv, relay_out, relay_in, res, sq_all,
    a_sem, w_sem, r_sem, g_sem, send_sem, recv_sem, rsend_sem, rrecv_sem, qsend_sem, qrecv_sem,
):
    chips = tp // CORES
    half = d_local // 2
    pp = half // COLS
    blk = 4 * pp
    tok_rows = a.shape[0]
    blocks = tok_rows // ROWS
    me = lax.axis_index("tp")
    chip, core = me // CORES, me % CORES

    def w_col(g):
        s, i = g % 2, (g % blk) // 2
        b, p, ph = i % 2, i // 2, g // blk
        is0 = (3 - ph) * (2 - ph) * (1 - ph) // 6
        is1 = ph * (3 - ph) * (2 - ph) // 2
        is2 = ph * (3 - ph) * (ph - 1) // 2
        kept = ph // 2
        step = 2 * s - 1
        hop = is0 * 2 + is1 * step + kept * (1 - b) * step
        to_core = (1 - kept) * b + is2 * (1 - core) + (kept - is2) * core
        in_half = s + is1 * (1 - 2 * s)
        to = ((chip + chips + hop) % chips) * CORES + to_core
        return to * d_local + in_half * half + p * COLS

    def w_copy(g):
        slot = g % W_SLOTS
        cols = pl.ds(pl.multiple_of(w_col(g), COLS), COLS)
        return pltpu.make_async_copy(w_hbm.at[:, cols], w.at[slot], w_sem.at[slot])

    def number(p, b, s):
        return (2 * p + b) * 2 + s

    def piece_copy(g):
        s, b, ph = g % 2, (g // 2) % 2, g // blk
        far = 1 - ph // 2
        to_chip = (chip + chips + far * (2 * s - 1)) % chips
        to_core = far * b + (1 - far) * (1 - core)
        slot = g + far * (core - b) * 2
        return pltpu.make_async_remote_copy(
            src_ref=part.at[g],
            dst_ref=recv.at[slot],
            send_sem=send_sem.at[g],
            recv_sem=recv_sem.at[slot],
            device_id={"tp": to_chip * CORES + to_core},
            device_id_type=pl.DeviceIdType.MESH,
        )

    def recv_wait(slot):
        pltpu.make_async_copy(recv.at[slot], recv.at[slot], recv_sem.at[slot]).wait()

    def relay_copy(j):
        to_chip = (chip + chips + 2 * (j % 2) - 1) % chips
        return pltpu.make_async_remote_copy(
            src_ref=relay_out.at[j],
            dst_ref=relay_in.at[j],
            send_sem=rsend_sem.at[j],
            recv_sem=rrecv_sem.at[j],
            device_id={"tp": to_chip * CORES + core},
            device_id_type=pl.DeviceIdType.MESH,
        )

    def sq_copy(j):
        return pltpu.make_async_remote_copy(
            src_ref=sq_all.at[me],
            dst_ref=sq_all.at[me],
            send_sem=qsend_sem.at[j],
            recv_sem=qrecv_sem.at[me],
            device_id={"tp": (me + j) % tp},
            device_id_type=pl.DeviceIdType.MESH,
        )

    a_copy = pltpu.make_async_copy(a_hbm, a, a_sem)
    r_copy = pltpu.make_async_copy(r_hbm, res, r_sem)
    g_copy = pltpu.make_async_copy(g_hbm, gain, g_sem)
    a_copy.start()
    w_copy(0).start()
    barrier = pltpu.get_barrier_semaphore()
    near = [chip * CORES + 1 - core]
    for hop in (1, chips - 1):
        near += [((chip + hop) % chips) * CORES + b for b in range(CORES)]
    for peer in near:
        pl.semaphore_signal(
            barrier, inc=1, device_id={"tp": peer}, device_id_type=pl.DeviceIdType.MESH
        )
    for g in range(1, W_SLOTS):
        w_copy(g).start()
    a_copy.wait()

    def project(g, carry):
        slot = g % W_SLOTS
        w_copy(g).wait()
        part[g] = jnp.dot(a[...], w[slot], preferred_element_type=jnp.float32).astype(jnp.bfloat16)

        @pl.when(g == 0)
        def _():
            pl.semaphore_wait(barrier, len(near))

        @pl.when(g < 3 * blk)
        def _():
            piece_copy(g).start()

        @pl.when(g + W_SLOTS < 4 * blk)
        def _():
            w_copy(g + W_SLOTS).start()

        return carry

    lax.fori_loop(0, 4 * blk, project, 0)
    r_copy.start()
    g_copy.start()

    def relay_wait(p, carry):
        for s in range(2):
            recv_wait(number(p, 0, s))
            recv_wait(number(p, 1, s))
            recv_wait(2 * blk + number(p, 0, s))
        return carry

    lax.fori_loop(0, pp, relay_wait, 0)

    def row_block(rb):
        return pl.ds(pl.multiple_of(rb * ROWS, ROWS), ROWS)

    def relay(j, carry):
        rows, s = row_block(j // 2), j % 2
        for p in range(pp):
            relay_out[j, :, p * COLS : (p + 1) * COLS] = (
                recv[number(p, 0, s), rows].astype(jnp.float32)
                + recv[number(p, 1, s), rows].astype(jnp.float32)
                + recv[2 * blk + number(p, 0, s), rows].astype(jnp.float32)
                + part[3 * blk + number(p, 0, s), rows].astype(jnp.float32)
            )
        relay_copy(j).start()
        return carry

    lax.fori_loop(0, 2 * blocks, relay, 0)
    r_copy.wait()

    def gather(i, carry):
        p, s = i // 2, i % 2
        cols = pl.ds(pl.multiple_of(s * half + p * COLS, COLS), COLS)
        direct = [blk + number(p, b, 1 - s) for b in range(CORES)]
        own = number(p, 1, s)
        for slot in direct:
            recv_wait(slot)
        recv_wait(2 * blk + own)
        hid[:, cols] = (
            res[:, cols].astype(jnp.float32)
            + part[3 * blk + own].astype(jnp.float32)
            + recv[2 * blk + own].astype(jnp.float32)
            + recv[direct[0]].astype(jnp.float32)
            + recv[direct[1]].astype(jnp.float32)
        )
        return carry

    lax.fori_loop(0, 2 * pp, gather, 0)

    for rb in range(blocks):
        rows = slice(rb * ROWS, (rb + 1) * ROWS)
        total = jnp.zeros((ROWS, 128), jnp.float32)
        for s in range(2):
            relay_copy(2 * rb + s).wait_recv()
            for c in range(0, half, 128):
                cols = slice(s * half + c, s * half + c + 128)
                h = hid[rows, cols] + relay_in[2 * rb + s, :, c : c + 128]
                hid[rows, cols] = h
                hid_bf[rows, cols] = h.astype(jnp.bfloat16)
                total += h * h
        sq_all[me, :, rows] = jnp.sum(jnp.transpose(total).reshape(16, 8, ROWS), axis=0)
    for j in range(1, tp):
        sq_copy(j).start()

    def drain(g, carry):
        piece_copy(g).wait_send()
        return carry

    lax.fori_loop(0, 3 * blk, drain, 0)
    for j in range(2 * blocks):
        relay_copy(j).wait_send()
    g_copy.wait()
    for j in range(1, tp):
        peer = (me + j) % tp
        pltpu.make_async_copy(sq_all.at[peer], sq_all.at[peer], qrecv_sem.at[peer]).wait()
    sq_sum[...] = jnp.sum(sq_all[...], axis=0)
    for j in range(1, tp):
        sq_copy(j).wait_send()


def norm_kernel(d_model, hid, hid_bf, sq_sum, gain, hid_out, nrm_out, nrm, sem):
    tok_rows, d_local = hid.shape
    hid_copy = pltpu.make_async_copy(hid_bf, hid_out, sem.at[0])
    hid_copy.start()
    sq_total = jnp.sum(sq_sum[...], axis=0, keepdims=True)
    scale_row = lax.rsqrt(sq_total / d_model + EPS)
    scale = jnp.transpose(jnp.broadcast_to(scale_row, (128, tok_rows)))
    copies = [hid_copy]
    for i, row in enumerate(range(0, tok_rows, OUT_ROWS)):
        rows = slice(row, row + OUT_ROWS)
        for c in range(0, d_local, 128):
            cols = slice(c, c + 128)
            nrm[rows, cols] = (hid[rows, cols] * scale[rows] * gain[:, cols]).astype(jnp.bfloat16)
        copies.append(pltpu.make_async_copy(nrm.at[rows], nrm_out.at[rows], sem.at[1 + i]))
        copies[-1].start()
    for copy in copies:
        copy.wait()


def solution(mesh):
    tp = mesh.shape["tp"]

    def local_step(attn_blk, w_blk, resid_blk, gain_blk):
        tok_rows, depth = attn_blk.shape
        d_local = resid_blk.shape[1]
        pp = d_local // 2 // COLS
        blocks = tok_rows // ROWS
        f32, bf16 = jnp.float32, jnp.bfloat16
        piece = (tok_rows, COLS)
        dma = pltpu.SemaphoreType.DMA
        hbm = pl.BlockSpec(memory_space=pl.ANY)
        vmem = pl.BlockSpec(memory_space=pltpu.VMEM)
        held = pl.pallas_call(
            functools.partial(reduce_kernel, tp, d_local),
            out_shape=[
                pltpu.VMEM((tok_rows, d_local), f32),
                pltpu.VMEM((tok_rows, d_local), bf16),
                pltpu.VMEM((8, tok_rows), f32),
                pltpu.VMEM((1, d_local), f32),
            ],
            in_specs=[hbm] * 4,
            out_specs=[vmem] * 4,
            scratch_shapes=[
                pltpu.VMEM((tok_rows, depth), bf16),
                pltpu.VMEM((W_SLOTS, depth, COLS), bf16),
                pltpu.VMEM((16 * pp, *piece), bf16),
                pltpu.VMEM((12 * pp, *piece), bf16),
                pltpu.VMEM((2 * blocks, ROWS, d_local // 2), f32),
                pltpu.VMEM((2 * blocks, ROWS, d_local // 2), f32),
                pltpu.VMEM((tok_rows, d_local), bf16),
                pltpu.VMEM((tp, 8, tok_rows), f32),
                dma,
                dma((W_SLOTS,)),
                dma,
                dma,
                dma((12 * pp,)),
                dma((12 * pp,)),
                dma((2 * blocks,)),
                dma((2 * blocks,)),
                dma((tp,)),
                dma((tp,)),
            ],
            compiler_params=pltpu.CompilerParams(
                collective_id=0, has_side_effects=True, vmem_limit_bytes=52 * 2**20
            ),
            name="project_reduce",
        )(attn_blk, w_blk, resid_blk, gain_blk.reshape(1, d_local))
        return pl.pallas_call(
            functools.partial(norm_kernel, tp * d_local),
            out_shape=[jax.ShapeDtypeStruct((tok_rows, d_local), bf16)] * 2,
            in_specs=[vmem] * 4,
            out_specs=[hbm] * 2,
            scratch_shapes=[
                pltpu.VMEM((tok_rows, d_local), bf16),
                dma((1 + tok_rows // OUT_ROWS,)),
            ],
            compiler_params=pltpu.CompilerParams(vmem_limit_bytes=16 * 2**20),
            name="norm_write",
        )(*held)

    return jax.shard_map(
        local_step,
        mesh=mesh,
        in_specs=(P("data", "tp"), P("tp", None), P("data", "tp"), P("tp")),
        out_specs=(P("data", "tp"), P("data", "tp")),
        check_vma=False,
    )
```

```python
import functools

import jax
import jax.numpy as jnp
from jax import lax
from jax.experimental import pallas as pl
from jax.experimental.pallas import tpu as pltpu
from jax.sharding import PartitionSpec as P

EPS = 1e-5
CORES = 2
COLS = 256
W_SLOTS = 6
ROWS = 64
OUT_ROWS = 64


def reduce_kernel(
    tp, d_local, a_hbm, w_hbm, r_hbm, g_hbm, hid, hid_bf, sq_sum, gain,
    a, w, part, recv, relay_out, relay_in, res, sq_all,
    a_sem, w_sem, r_sem, g_sem, send_sem, mid_sem, end_sem, rsend_sem, rrecv_sem, q_sem,
):
    chips = tp // CORES
    half = d_local // 2
    pp = half // COLS
    blk = 4 * pp
    tok_rows = a.shape[0]
    blocks = tok_rows // ROWS
    me = lax.axis_index("tp")
    chip, core = me // CORES, me % CORES

    def w_col(g):
        s, i = g % 2, (g % blk) // 2
        b, p, ph = i % 2, i // 2, g // blk
        is0 = (3 - ph) * (2 - ph) * (1 - ph) // 6
        is1 = ph * (3 - ph) * (2 - ph) // 2
        is2 = ph * (3 - ph) * (ph - 1) // 2
        kept = ph // 2
        step = 2 * s - 1
        hop = is0 * 2 + is1 * step + kept * (1 - b) * step
        mine = (kept - is2) * b + is2 * (1 - b)
        to_core = (1 - kept) * b + kept * (mine * core + (1 - mine) * (1 - core))
        in_half = s + is1 * (1 - 2 * s)
        to = ((chip + chips + hop) % chips) * CORES + to_core
        return to * d_local + in_half * half + p * COLS

    def w_copy(g):
        slot = g % W_SLOTS
        cols = pl.ds(pl.multiple_of(w_col(g), COLS), COLS)
        return pltpu.make_async_copy(w_hbm.at[:, cols], w.at[slot], w_sem.at[slot])

    def number(p, b, s):
        return (2 * p + b) * 2 + s

    def piece_copy(g, sem, rows=slice(None)):
        s, b, ph = g % 2, (g // 2) % 2, g // blk
        far = 1 - ph // 2
        direct = far * ph
        to_chip = (chip + chips + far * (2 * s - 1)) % chips
        to_core = direct * b + (far - direct) * (1 - b) + (1 - far) * (1 - core)
        slot = g + far * (core - b) * 2
        return pltpu.make_async_remote_copy(
            src_ref=part.at[g, rows],
            dst_ref=recv.at[slot, rows],
            send_sem=send_sem,
            recv_sem=sem,
            device_id={"tp": to_chip * CORES + to_core},
            device_id_type=pl.DeviceIdType.MESH,
        )

    def wait_for(ref, sem):
        pltpu.make_async_copy(ref, ref, sem).wait()

    def relay_copy(j):
        to_chip = (chip + chips + 2 * (j % 2) - 1) % chips
        return pltpu.make_async_remote_copy(
            src_ref=relay_out.at[j],
            dst_ref=relay_in.at[j],
            send_sem=rsend_sem,
            recv_sem=rrecv_sem.at[j],
            device_id={"tp": to_chip * CORES + 1 - core},
            device_id_type=pl.DeviceIdType.MESH,
        )

    def sq_copy(j):
        return pltpu.make_async_remote_copy(
            src_ref=sq_all.at[me],
            dst_ref=sq_all.at[me],
            send_sem=q_sem.at[0],
            recv_sem=q_sem.at[1],
            device_id={"tp": (me + j) % tp},
            device_id_type=pl.DeviceIdType.MESH,
        )

    top, low = slice(0, tok_rows // 2), slice(tok_rows // 2, tok_rows)
    a_copies = [
        pltpu.make_async_copy(a_hbm.at[rows], a.at[rows], a_sem.at[i])
        for i, rows in enumerate((top, low))
    ]
    r_copy = pltpu.make_async_copy(r_hbm, res, r_sem)
    g_copy = pltpu.make_async_copy(g_hbm, gain, g_sem)
    a_copies[0].start()
    w_copy(0).start()
    w_copy(1).start()
    a_copies[1].start()
    barrier = pltpu.get_barrier_semaphore()
    near = [chip * CORES + 1 - core]
    for hop in (1, chips - 1):
        near += [((chip + hop) % chips) * CORES + b for b in range(CORES)]
    for peer in near:
        pl.semaphore_signal(
            barrier, inc=1, device_id={"tp": peer}, device_id_type=pl.DeviceIdType.MESH
        )
    for g in range(2, W_SLOTS):
        w_copy(g).start()

    def project(g, rows=slice(None)):
        part[g, rows] = jnp.dot(
            a[rows], w[g % W_SLOTS], preferred_element_type=jnp.float32
        ).astype(jnp.bfloat16)

    for i, rows in enumerate((top, low)):
        a_copies[i].wait()
        for g in range(2):
            if i == 0:
                w_copy(g).wait()
            project(g, rows)
            if i == 0 and g == 0:
                pl.semaphore_wait(barrier, len(near))
            piece_copy(g, mid_sem, rows).start()
    for g in range(2):
        w_copy(W_SLOTS + g).start()

    def step(g, carry):
        w_copy(g).wait()
        project(g)
        b, ph = (g // 2) % 2, g // blk
        for_end = ph % 2 + ph // 2 * b

        @pl.when((g < 3 * blk) & (for_end == 0))
        def _():
            piece_copy(g, mid_sem).start()

        @pl.when((g < 3 * blk) & (for_end == 1))
        def _():
            piece_copy(g, end_sem).start()

        @pl.when(g + W_SLOTS < 4 * blk)
        def _():
            w_copy(g + W_SLOTS).start()

        return carry

    lax.fori_loop(2, 4 * blk, step, 0)
    r_copy.start()
    g_copy.start()
    wait_for(recv.at[pl.ds(0, blk + blk // 2)], mid_sem)

    def row_block(rb):
        return pl.ds(pl.multiple_of(rb * ROWS, ROWS), ROWS)

    def relay(j, carry):
        rows, s = row_block(j // 2), j % 2
        for p in range(pp):
            relay_out[j, :, p * COLS : (p + 1) * COLS] = (
                recv[number(p, 0, s), rows].astype(jnp.float32)
                + recv[number(p, 1, s), rows].astype(jnp.float32)
                + recv[2 * blk + number(p, 0, s), rows].astype(jnp.float32)
                + part[3 * blk + number(p, 0, s), rows].astype(jnp.float32)
            )
        relay_copy(j).start()
        return carry

    lax.fori_loop(0, 2 * blocks, relay, 0)
    r_copy.wait()
    wait_for(recv.at[pl.ds(0, blk + blk // 2)], end_sem)

    def gather(i, carry):
        p, s = i // 2, i % 2
        cols = pl.ds(pl.multiple_of(s * half + p * COLS, COLS), COLS)
        direct = [blk + number(p, b, 1 - s) for b in range(CORES)]
        own = number(p, 1, s)
        hid[:, cols] = (
            res[:, cols].astype(jnp.float32)
            + part[3 * blk + own].astype(jnp.float32)
            + recv[2 * blk + own].astype(jnp.float32)
            + recv[direct[0]].astype(jnp.float32)
            + recv[direct[1]].astype(jnp.float32)
        )
        return carry

    lax.fori_loop(0, 2 * pp, gather, 0)

    totals = []
    for rb in range(blocks):
        rows = slice(rb * ROWS, (rb + 1) * ROWS)
        total = jnp.zeros((ROWS, 128), jnp.float32)
        for s in range(2):
            relay_copy(2 * rb + s).wait_recv()
            for c in range(0, half, 128):
                cols = slice(s * half + c, s * half + c + 128)
                h = hid[rows, cols] + relay_in[2 * rb + s, :, c : c + 128]
                hid[rows, cols] = h
                total += h * h
        totals.append(total)
        if len(totals) * ROWS == 128:
            by_lane = jnp.transpose(jnp.concatenate(totals, axis=0))
            sq_all[me, :, (rb + 1) * ROWS - 128 : (rb + 1) * ROWS] = jnp.sum(
                by_lane.reshape(16, 8, 128), axis=0
            )
            totals = []
    for j in range(1, tp):
        sq_copy(j).start()

    def narrow(rb, carry):
        rows = row_block(rb)
        hid_bf[rows] = hid[rows].astype(jnp.bfloat16)
        return carry

    lax.fori_loop(0, blocks, narrow, 0)
    wait_for(part.at[pl.ds(0, 3 * blk)], send_sem)
    wait_for(relay_out, rsend_sem)
    g_copy.wait()
    wait_for(sq_all.at[pl.ds(0, tp - 1)], q_sem.at[1])
    sq_sum[...] = jnp.sum(sq_all[...], axis=0)
    wait_for(sq_all.at[pl.ds(0, tp - 1)], q_sem.at[0])


def norm_kernel(d_model, hid, hid_bf, sq_sum, gain, hid_out, nrm_out, nrm, sem):
    tok_rows, d_local = hid.shape
    hid_copy = pltpu.make_async_copy(hid_bf, hid_out, sem.at[0])
    hid_copy.start()
    sq_total = jnp.sum(sq_sum[...], axis=0, keepdims=True)
    scale_row = lax.rsqrt(sq_total / d_model + EPS)
    scale = jnp.transpose(jnp.broadcast_to(scale_row, (128, tok_rows)))
    copies = [hid_copy]
    for i, row in enumerate(range(0, tok_rows, OUT_ROWS)):
        rows = slice(row, row + OUT_ROWS)
        for c in range(0, d_local, 128):
            cols = slice(c, c + 128)
            nrm[rows, cols] = (hid[rows, cols] * scale[rows] * gain[:, cols]).astype(jnp.bfloat16)
        copies.append(pltpu.make_async_copy(nrm.at[rows], nrm_out.at[rows], sem.at[1 + i]))
        copies[-1].start()
    for copy in copies:
        copy.wait()


def solution(mesh):
    tp = mesh.shape["tp"]

    def local_step(attn_blk, w_blk, resid_blk, gain_blk):
        tok_rows, depth = attn_blk.shape
        d_local = resid_blk.shape[1]
        pp = d_local // 2 // COLS
        blocks = tok_rows // ROWS
        f32, bf16 = jnp.float32, jnp.bfloat16
        piece = (tok_rows, COLS)
        dma = pltpu.SemaphoreType.DMA
        hbm = pl.BlockSpec(memory_space=pl.ANY)
        vmem = pl.BlockSpec(memory_space=pltpu.VMEM)
        held = pl.pallas_call(
            functools.partial(reduce_kernel, tp, d_local),
            out_shape=[
                pltpu.VMEM((tok_rows, d_local), f32),
                pltpu.VMEM((tok_rows, d_local), bf16),
                pltpu.VMEM((8, tok_rows), f32),
                pltpu.VMEM((1, d_local), f32),
            ],
            in_specs=[hbm] * 4,
            out_specs=[vmem] * 4,
            scratch_shapes=[
                pltpu.VMEM((tok_rows, depth), bf16),
                pltpu.VMEM((W_SLOTS, depth, COLS), bf16),
                pltpu.VMEM((16 * pp, *piece), bf16),
                pltpu.VMEM((12 * pp, *piece), bf16),
                pltpu.VMEM((2 * blocks, ROWS, d_local // 2), f32),
                pltpu.VMEM((2 * blocks, ROWS, d_local // 2), f32),
                pltpu.VMEM((tok_rows, d_local), bf16),
                pltpu.VMEM((tp, 8, tok_rows), f32),
                dma((2,)),
                dma((W_SLOTS,)),
                dma,
                dma,
                dma,
                dma,
                dma,
                dma,
                dma((2 * blocks,)),
                dma((2,)),
            ],
            compiler_params=pltpu.CompilerParams(
                collective_id=0, has_side_effects=True, vmem_limit_bytes=52 * 2**20
            ),
            name="project_reduce",
        )(attn_blk, w_blk, resid_blk, gain_blk.reshape(1, d_local))
        return pl.pallas_call(
            functools.partial(norm_kernel, tp * d_local),
            out_shape=[jax.ShapeDtypeStruct((tok_rows, d_local), bf16)] * 2,
            in_specs=[vmem] * 4,
            out_specs=[hbm] * 2,
            scratch_shapes=[
                pltpu.VMEM((tok_rows, d_local), bf16),
                dma((1 + tok_rows // OUT_ROWS,)),
            ],
            compiler_params=pltpu.CompilerParams(vmem_limit_bytes=16 * 2**20),
            name="norm_write",
        )(*held)

    return jax.shard_map(
        local_step,
        mesh=mesh,
        in_specs=(P("data", "tp"), P("tp", None), P("data", "tp"), P("tp")),
        out_specs=(P("data", "tp"), P("data", "tp")),
        check_vma=False,
    )
```

```python
import functools

import jax
import jax.numpy as jnp
from jax import lax
from jax.experimental import pallas as pl
from jax.experimental.pallas import tpu as pltpu
from jax.sharding import PartitionSpec as P

EPS = 1e-5
CORES = 2
COLS = 256
W_SLOTS = 6
ROWS = 64
OUT_ROWS = 64


def reduce_kernel(
    tp, d_local, a_hbm, w_hbm, r_hbm, g_hbm, hid, hid_bf, sq_sum, gain,
    a, w, part, recv, relay_out, relay_in, res, sq_all,
    a_sem, w_sem, r_sem, g_sem, send_sem, mid_sem, end_sem, rsend_sem, rrecv_sem, q_sem,
):
    chips = tp // CORES
    half = d_local // 2
    pp = half // COLS
    blk = 4 * pp
    tok_rows = a.shape[0]
    blocks = tok_rows // ROWS
    me = lax.axis_index("tp")
    chip, core = me // CORES, me % CORES

    def w_col(g):
        s, i = g % 2, (g % blk) // 2
        b, p, ph = i % 2, i // 2, g // blk
        is0 = (3 - ph) * (2 - ph) * (1 - ph) // 6
        is1 = ph * (3 - ph) * (2 - ph) // 2
        is2 = ph * (3 - ph) * (ph - 1) // 2
        kept = ph // 2
        step = 1 - 2 * s
        hop = is0 * 2 + is1 * step + kept * (1 - b) * step
        mine = (kept - is2) * b + is2 * (1 - b)
        to_core = (1 - kept) * b + kept * (mine * core + (1 - mine) * (1 - core))
        in_half = s + is1 * (1 - 2 * s)
        to = ((chip + chips + hop) % chips) * CORES + to_core
        return to * d_local + in_half * half + p * COLS

    def w_copy(g):
        slot = g % W_SLOTS
        cols = pl.ds(pl.multiple_of(w_col(g), COLS), COLS)
        return pltpu.make_async_copy(w_hbm.at[:, cols], w.at[slot], w_sem.at[slot])

    def number(p, b, s):
        return (2 * p + b) * 2 + s

    def piece_copy(g, sem, rows=slice(None)):
        s, b, ph = g % 2, (g // 2) % 2, g // blk
        far = 1 - ph // 2
        direct = far * ph
        to_chip = (chip + chips + far * (1 - 2 * s)) % chips
        to_core = direct * b + (far - direct) * (1 - b) + (1 - far) * (1 - core)
        slot = g + far * (core - b) * 2
        return pltpu.make_async_remote_copy(
            src_ref=part.at[g, rows],
            dst_ref=recv.at[slot, rows],
            send_sem=send_sem,
            recv_sem=sem,
            device_id={"tp": to_chip * CORES + to_core},
            device_id_type=pl.DeviceIdType.MESH,
        )

    def wait_for(ref, sem):
        pltpu.make_async_copy(ref, ref, sem).wait()

    def relay_copy(j):
        to_chip = (chip + chips + 1 - 2 * (j % 2)) % chips
        return pltpu.make_async_remote_copy(
            src_ref=relay_out.at[j],
            dst_ref=relay_in.at[j],
            send_sem=rsend_sem,
            recv_sem=rrecv_sem.at[j],
            device_id={"tp": to_chip * CORES + 1 - core},
            device_id_type=pl.DeviceIdType.MESH,
        )

    def peers(hops):
        return [((chip + hop) % chips) * CORES + b for hop in hops for b in range(CORES)]

    partner = chip * CORES + 1 - core
    others = sorted(range(1, chips), key=lambda hop: -min(hop, chips - hop))

    def sq_copy(peer):
        return pltpu.make_async_remote_copy(
            src_ref=sq_all.at[me],
            dst_ref=sq_all.at[me],
            send_sem=q_sem.at[0],
            recv_sem=q_sem.at[1],
            device_id={"tp": peer},
            device_id_type=pl.DeviceIdType.MESH,
        )

    top, low = slice(0, tok_rows // 2), slice(tok_rows // 2, tok_rows)
    a_copies = [
        pltpu.make_async_copy(a_hbm.at[rows], a.at[rows], a_sem.at[i])
        for i, rows in enumerate((top, low))
    ]
    r_copy = pltpu.make_async_copy(r_hbm, res, r_sem)
    g_copy = pltpu.make_async_copy(g_hbm, gain, g_sem)
    barrier = pltpu.get_barrier_semaphore()
    near = peers((1, chips - 1)) + [partner]
    for peer in near:
        pl.semaphore_signal(
            barrier, inc=1, device_id={"tp": peer}, device_id_type=pl.DeviceIdType.MESH
        )
    a_copies[0].start()
    w_copy(0).start()
    w_copy(1).start()
    a_copies[1].start()
    for g in range(2, W_SLOTS):
        w_copy(g).start()

    def project(g, rows=slice(None)):
        part[g, rows] = jnp.dot(
            a[rows], w[g % W_SLOTS], preferred_element_type=jnp.float32
        ).astype(jnp.bfloat16)

    for i, rows in enumerate((top, low)):
        a_copies[i].wait()
        for g in range(2):
            if i == 0:
                w_copy(g).wait()
            project(g, rows)
            if i == 0 and g == 0:
                pl.semaphore_wait(barrier, len(near))
            piece_copy(g, mid_sem, rows).start()
    for g in range(2):
        w_copy(W_SLOTS + g).start()

    def step(g, carry):
        w_copy(g).wait()
        project(g)
        b, ph = (g // 2) % 2, g // blk
        for_end = ph % 2 + ph // 2 * b

        @pl.when((g < 3 * blk) & (for_end == 0))
        def _():
            piece_copy(g, mid_sem).start()

        @pl.when((g < 3 * blk) & (for_end == 1))
        def _():
            piece_copy(g, end_sem).start()

        @pl.when(g + W_SLOTS < 4 * blk)
        def _():
            w_copy(g + W_SLOTS).start()

        return carry

    lax.fori_loop(2, 4 * blk, step, 0)
    r_copy.start()
    g_copy.start()
    wait_for(recv.at[pl.ds(0, blk + blk // 2)], mid_sem)

    def row_block(rb):
        return pl.ds(pl.multiple_of(rb * ROWS, ROWS), ROWS)

    def relay(j, carry):
        rows, s = row_block(j // 2), j % 2
        for p in range(pp):
            relay_out[j, :, p * COLS : (p + 1) * COLS] = (
                recv[number(p, 0, s), rows].astype(jnp.float32)
                + recv[number(p, 1, s), rows].astype(jnp.float32)
                + recv[2 * blk + number(p, 0, s), rows].astype(jnp.float32)
                + part[3 * blk + number(p, 0, s), rows].astype(jnp.float32)
            )
        relay_copy(j).start()
        return carry

    lax.fori_loop(0, 2 * blocks, relay, 0)
    r_copy.wait()
    wait_for(recv.at[pl.ds(0, blk + blk // 2)], end_sem)

    def gather(i, carry):
        p, s = i // 2, i % 2
        cols = pl.ds(pl.multiple_of(s * half + p * COLS, COLS), COLS)
        direct = [blk + number(p, b, 1 - s) for b in range(CORES)]
        own = number(p, 1, s)
        hid[:, cols] = (
            res[:, cols].astype(jnp.float32)
            + part[3 * blk + own].astype(jnp.float32)
            + recv[2 * blk + own].astype(jnp.float32)
            + recv[direct[0]].astype(jnp.float32)
            + recv[direct[1]].astype(jnp.float32)
        )
        return carry

    lax.fori_loop(0, 2 * pp, gather, 0)

    totals = []
    for rb in range(blocks):
        rows = slice(rb * ROWS, (rb + 1) * ROWS)
        total = jnp.zeros((ROWS, 128), jnp.float32)
        for s in range(2):
            relay_copy(2 * rb + s).wait_recv()
            for c in range(0, half, 128):
                cols = slice(s * half + c, s * half + c + 128)
                h = hid[rows, cols] + relay_in[2 * rb + s, :, c : c + 128]
                hid[rows, cols] = h
                total += h * h
        totals.append(total)
        if len(totals) * ROWS == 128:
            by_lane = jnp.transpose(jnp.concatenate(totals, axis=0))
            sq_all[me, :, (rb + 1) * ROWS - 128 : (rb + 1) * ROWS] = jnp.sum(
                by_lane, axis=0, keepdims=True
            )
            totals = []
    for peer in peers(others) + [partner]:
        sq_copy(peer).start()

    def narrow(rb, carry):
        rows = row_block(rb)
        hid_bf[rows] = hid[rows].astype(jnp.bfloat16)
        return carry

    lax.fori_loop(0, blocks, narrow, 0)
    wait_for(part.at[pl.ds(0, 3 * blk)], send_sem)
    wait_for(relay_out, rsend_sem)
    g_copy.wait()
    wait_for(sq_all.at[pl.ds(0, tp - 1)], q_sem.at[1])
    sq_sum[...] = jnp.sum(sq_all[...], axis=0)
    wait_for(sq_all.at[pl.ds(0, tp - 1)], q_sem.at[0])


def norm_kernel(d_model, hid, hid_bf, sq_sum, gain, hid_out, nrm_out, nrm, sem):
    tok_rows, d_local = hid.shape
    hid_copy = pltpu.make_async_copy(hid_bf, hid_out, sem.at[0])
    hid_copy.start()
    scale_row = lax.rsqrt(sq_sum[...] / d_model + EPS)
    scale = jnp.transpose(jnp.broadcast_to(scale_row, (128, tok_rows)))
    copies = [hid_copy]
    for i, row in enumerate(range(0, tok_rows, OUT_ROWS)):
        rows = slice(row, row + OUT_ROWS)
        for c in range(0, d_local, 128):
            cols = slice(c, c + 128)
            nrm[rows, cols] = (hid[rows, cols] * scale[rows] * gain[:, cols]).astype(jnp.bfloat16)
        copies.append(pltpu.make_async_copy(nrm.at[rows], nrm_out.at[rows], sem.at[1 + i]))
        copies[-1].start()
    for copy in copies:
        copy.wait()


def solution(mesh):
    tp = mesh.shape["tp"]

    def local_step(attn_blk, w_blk, resid_blk, gain_blk):
        tok_rows, depth = attn_blk.shape
        d_local = resid_blk.shape[1]
        pp = d_local // 2 // COLS
        blocks = tok_rows // ROWS
        f32, bf16 = jnp.float32, jnp.bfloat16
        piece = (tok_rows, COLS)
        dma = pltpu.SemaphoreType.DMA
        hbm = pl.BlockSpec(memory_space=pl.ANY)
        vmem = pl.BlockSpec(memory_space=pltpu.VMEM)
        held = pl.pallas_call(
            functools.partial(reduce_kernel, tp, d_local),
            out_shape=[
                pltpu.VMEM((tok_rows, d_local), f32),
                pltpu.VMEM((tok_rows, d_local), bf16),
                pltpu.VMEM((1, tok_rows), f32),
                pltpu.VMEM((1, d_local), f32),
            ],
            in_specs=[hbm] * 4,
            out_specs=[vmem] * 4,
            scratch_shapes=[
                pltpu.VMEM((tok_rows, depth), bf16),
                pltpu.VMEM((W_SLOTS, depth, COLS), bf16),
                pltpu.VMEM((16 * pp, *piece), bf16),
                pltpu.VMEM((12 * pp, *piece), bf16),
                pltpu.VMEM((2 * blocks, ROWS, d_local // 2), f32),
                pltpu.VMEM((2 * blocks, ROWS, d_local // 2), f32),
                pltpu.VMEM((tok_rows, d_local), bf16),
                pltpu.VMEM((tp, 1, tok_rows), f32),
                dma((2,)),
                dma((W_SLOTS,)),
                dma,
                dma,
                dma,
                dma,
                dma,
                dma,
                dma((2 * blocks,)),
                dma((2,)),
            ],
            compiler_params=pltpu.CompilerParams(
                collective_id=0, has_side_effects=True, vmem_limit_bytes=52 * 2**20
            ),
            name="project_reduce",
        )(attn_blk, w_blk, resid_blk, gain_blk.reshape(1, d_local))
        return pl.pallas_call(
            functools.partial(norm_kernel, tp * d_local),
            out_shape=[jax.ShapeDtypeStruct((tok_rows, d_local), bf16)] * 2,
            in_specs=[vmem] * 4,
            out_specs=[hbm] * 2,
            scratch_shapes=[
                pltpu.VMEM((tok_rows, d_local), bf16),
                dma((1 + tok_rows // OUT_ROWS,)),
            ],
            compiler_params=pltpu.CompilerParams(vmem_limit_bytes=16 * 2**20),
            name="norm_write",
        )(*held)

    return jax.shard_map(
        local_step,
        mesh=mesh,
        in_specs=(P("data", "tp"), P("tp", None), P("data", "tp"), P("tp")),
        out_specs=(P("data", "tp"), P("data", "tp")),
        check_vma=False,
    )
```

```python
import functools

import jax
import jax.numpy as jnp
from jax import lax
from jax.experimental import pallas as pl
from jax.experimental.pallas import tpu as pltpu
from jax.sharding import PartitionSpec as P

EPS = 1e-5
CORES = 2
COLS = 256
W_SLOTS = 6
ROWS = 64
OUT_ROWS = 64


def reduce_kernel(
    tp, d_local, a_hbm, w_hbm, r_hbm, g_hbm, hid, hid_bf, sq_sum, gain,
    a, w, part, recv, relay_out, relay_in, res, sq_all,
    a_sem, w_sem, r_sem, g_sem, send_sem, mid_sem, end_sem, rsend_sem, rrecv_sem, q_sem,
):
    chips = tp // CORES
    half = d_local // 2
    pp = half // COLS
    blk = 4 * pp
    mix = COLS // 2
    tok_rows = a.shape[0]
    blocks = tok_rows // ROWS
    me = lax.axis_index("tp")
    chip, core = me // CORES, me % CORES

    def w_col(g):
        s, i = g % 2, (g % blk) // 2
        b, p, ph = i % 2, i // 2, g // blk
        is0 = (3 - ph) * (2 - ph) * (1 - ph) // 6
        is1 = ph * (3 - ph) * (2 - ph) // 2
        is2 = ph * (3 - ph) * (ph - 1) // 2
        kept = ph // 2
        step = 2 * s - 1
        hop = is0 * 2 + is1 * step + kept * (1 - b) * step
        mine = (kept - is2) * b + is2 * (1 - b)
        to_core = (1 - kept) * b + kept * (mine * core + (1 - mine) * (1 - core))
        in_half = s + is1 * (1 - 2 * s)
        to = ((chip + chips + hop) % chips) * CORES + to_core
        return to * d_local + in_half * half + p * COLS

    def w_copy(g):
        slot = g % W_SLOTS
        cols = pl.ds(pl.multiple_of(w_col(g), COLS), COLS)
        return pltpu.make_async_copy(w_hbm.at[:, cols], w.at[slot], w_sem.at[slot])

    def mixed_copies(i):
        return [
            pltpu.make_async_copy(
                w_hbm.at[:, pl.ds(pl.multiple_of(w_col(g) + i * mix, mix), mix)],
                w.at[i, :, pl.ds(g * mix, mix)],
                w_sem.at[i],
            )
            for g in range(2)
        ]

    def number(p, b, s):
        return (2 * p + b) * 2 + s

    def piece_copy(g, sem, rows=slice(None), cols=slice(None)):
        s, b, ph = g % 2, (g // 2) % 2, g // blk
        far = 1 - ph // 2
        direct = far * ph
        to_chip = (chip + chips + far * (2 * s - 1)) % chips
        to_core = direct * b + (far - direct) * (1 - b) + (1 - far) * (1 - core)
        slot = g + far * (core - b) * 2
        return pltpu.make_async_remote_copy(
            src_ref=part.at[g, rows, cols],
            dst_ref=recv.at[slot, rows, cols],
            send_sem=send_sem,
            recv_sem=sem,
            device_id={"tp": to_chip * CORES + to_core},
            device_id_type=pl.DeviceIdType.MESH,
        )

    def wait_for(ref, sem):
        pltpu.make_async_copy(ref, ref, sem).wait()

    def relay_copy(j):
        to_chip = (chip + chips + 2 * (j % 2) - 1) % chips
        return pltpu.make_async_remote_copy(
            src_ref=relay_out.at[j],
            dst_ref=relay_in.at[j],
            send_sem=rsend_sem,
            recv_sem=rrecv_sem.at[j],
            device_id={"tp": to_chip * CORES + 1 - core},
            device_id_type=pl.DeviceIdType.MESH,
        )

    def peers(hops):
        return [((chip + hop) % chips) * CORES + b for hop in hops for b in range(CORES)]

    partner = chip * CORES + 1 - core
    others = sorted(range(1, chips), key=lambda hop: -min(hop, chips - hop))

    def sq_copy(peer):
        return pltpu.make_async_remote_copy(
            src_ref=sq_all.at[me],
            dst_ref=sq_all.at[me],
            send_sem=q_sem.at[0],
            recv_sem=q_sem.at[1],
            device_id={"tp": peer},
            device_id_type=pl.DeviceIdType.MESH,
        )

    top, low = slice(0, tok_rows // 2), slice(tok_rows // 2, tok_rows)
    a_copies = [
        pltpu.make_async_copy(a_hbm.at[rows], a.at[rows], a_sem.at[i])
        for i, rows in enumerate((top, low))
    ]
    r_copy = pltpu.make_async_copy(r_hbm, res, r_sem)
    g_copy = pltpu.make_async_copy(g_hbm, gain, g_sem)
    a_copies[0].start()
    for copy in mixed_copies(0):
        copy.start()
    a_copies[1].start()
    for copy in mixed_copies(1):
        copy.start()
    barrier = pltpu.get_barrier_semaphore()
    near = [partner] + peers((1, chips - 1))
    for peer in near:
        pl.semaphore_signal(
            barrier, inc=1, device_id={"tp": peer}, device_id_type=pl.DeviceIdType.MESH
        )
    for g in range(2, W_SLOTS):
        w_copy(g).start()

    for i in range(2):
        for j, rows in enumerate((top, low)):
            if i == 0:
                a_copies[j].wait()
            if j == 0:
                wait_for(w.at[i], w_sem.at[i])
            quarter = jnp.dot(a[rows], w[i], preferred_element_type=jnp.float32)
            for g in range(2):
                cols = slice(i * mix, (i + 1) * mix)
                part[g, rows, cols] = quarter[:, g * mix : (g + 1) * mix].astype(jnp.bfloat16)
            if i == 0 and j == 0:
                pl.semaphore_wait(barrier, len(near))
            for g in range(2):
                piece_copy(g, mid_sem, rows, cols).start()
    for g in range(2):
        w_copy(W_SLOTS + g).start()

    def step(g, carry):
        slot = g % W_SLOTS
        w_copy(g).wait()
        part[g] = jnp.dot(a[...], w[slot], preferred_element_type=jnp.float32).astype(jnp.bfloat16)
        b, ph = (g // 2) % 2, g // blk
        for_end = ph % 2 + ph // 2 * b

        @pl.when((g < 3 * blk) & (for_end == 0))
        def _():
            piece_copy(g, mid_sem).start()

        @pl.when((g < 3 * blk) & (for_end == 1))
        def _():
            piece_copy(g, end_sem).start()

        @pl.when(g + W_SLOTS < 4 * blk)
        def _():
            w_copy(g + W_SLOTS).start()

        return carry

    lax.fori_loop(2, 4 * blk, step, 0)
    r_copy.start()
    g_copy.start()
    wait_for(recv.at[pl.ds(0, blk + blk // 2)], mid_sem)

    def row_block(rb):
        return pl.ds(pl.multiple_of(rb * ROWS, ROWS), ROWS)

    def relay(j, carry):
        rows, s = row_block(j // 2), j % 2
        for p in range(pp):
            relay_out[j, :, p * COLS : (p + 1) * COLS] = (
                recv[number(p, 0, s), rows].astype(jnp.float32)
                + recv[number(p, 1, s), rows].astype(jnp.float32)
                + recv[2 * blk + number(p, 0, s), rows].astype(jnp.float32)
                + part[3 * blk + number(p, 0, s), rows].astype(jnp.float32)
            )
        relay_copy(j).start()
        return carry

    lax.fori_loop(0, 2 * blocks, relay, 0)
    r_copy.wait()
    wait_for(recv.at[pl.ds(0, blk + blk // 2)], end_sem)

    def gather(i, carry):
        p, s = i // 2, i % 2
        cols = pl.ds(pl.multiple_of(s * half + p * COLS, COLS), COLS)
        direct = [blk + number(p, b, 1 - s) for b in range(CORES)]
        own = number(p, 1, s)
        hid[:, cols] = (
            res[:, cols].astype(jnp.float32)
            + part[3 * blk + own].astype(jnp.float32)
            + recv[2 * blk + own].astype(jnp.float32)
            + recv[direct[0]].astype(jnp.float32)
            + recv[direct[1]].astype(jnp.float32)
        )
        return carry

    lax.fori_loop(0, 2 * pp, gather, 0)

    totals = []
    for rb in range(blocks):
        rows = slice(rb * ROWS, (rb + 1) * ROWS)
        total = jnp.zeros((ROWS, 128), jnp.float32)
        for s in range(2):
            relay_copy(2 * rb + s).wait_recv()
            for c in range(0, half, 128):
                cols = slice(s * half + c, s * half + c + 128)
                h = hid[rows, cols] + relay_in[2 * rb + s, :, c : c + 128]
                hid[rows, cols] = h
                total += h * h
        totals.append(total)
        if len(totals) * ROWS == 128:
            by_lane = jnp.transpose(jnp.concatenate(totals, axis=0))
            sq_all[me, :, (rb + 1) * ROWS - 128 : (rb + 1) * ROWS] = jnp.sum(
                by_lane, axis=0, keepdims=True
            )
            totals = []
    for peer in peers(others) + [partner]:
        sq_copy(peer).start()

    def narrow(rb, carry):
        rows = row_block(rb)
        hid_bf[rows] = hid[rows].astype(jnp.bfloat16)
        return carry

    lax.fori_loop(0, blocks, narrow, 0)
    wait_for(part.at[pl.ds(0, 3 * blk)], send_sem)
    wait_for(relay_out, rsend_sem)
    g_copy.wait()
    wait_for(sq_all.at[pl.ds(0, tp - 1)], q_sem.at[1])
    sq_sum[...] = jnp.sum(sq_all[...], axis=0)
    wait_for(sq_all.at[pl.ds(0, tp - 1)], q_sem.at[0])


def norm_kernel(d_model, hid, hid_bf, sq_sum, gain, hid_out, nrm_out, nrm, sem):
    tok_rows, d_local = hid.shape
    copies = []

    def write(src, dst, rows):
        copies.append(pltpu.make_async_copy(src.at[rows], dst.at[rows], sem.at[len(copies)]))
        copies[-1].start()

    blocks = [slice(row, row + OUT_ROWS) for row in range(0, tok_rows, OUT_ROWS)]
    for rows in blocks:
        write(hid_bf, hid_out, rows)
    scale_row = lax.rsqrt(sq_sum[...] / d_model + EPS)
    scale = jnp.transpose(jnp.broadcast_to(scale_row, (128, tok_rows)))
    for rows in blocks:
        for c in range(0, d_local, 128):
            cols = slice(c, c + 128)
            nrm[rows, cols] = (hid[rows, cols] * scale[rows] * gain[:, cols]).astype(jnp.bfloat16)
        write(nrm, nrm_out, rows)
    for copy in copies:
        copy.wait()


def solution(mesh):
    tp = mesh.shape["tp"]

    def local_step(attn_blk, w_blk, resid_blk, gain_blk):
        tok_rows, depth = attn_blk.shape
        d_local = resid_blk.shape[1]
        pp = d_local // 2 // COLS
        blocks = tok_rows // ROWS
        f32, bf16 = jnp.float32, jnp.bfloat16
        piece = (tok_rows, COLS)
        dma = pltpu.SemaphoreType.DMA
        hbm = pl.BlockSpec(memory_space=pl.ANY)
        vmem = pl.BlockSpec(memory_space=pltpu.VMEM)
        held = pl.pallas_call(
            functools.partial(reduce_kernel, tp, d_local),
            out_shape=[
                pltpu.VMEM((tok_rows, d_local), f32),
                pltpu.VMEM((tok_rows, d_local), bf16),
                pltpu.VMEM((1, tok_rows), f32),
                pltpu.VMEM((1, d_local), f32),
            ],
            in_specs=[hbm] * 4,
            out_specs=[vmem] * 4,
            scratch_shapes=[
                pltpu.VMEM((tok_rows, depth), bf16),
                pltpu.VMEM((W_SLOTS, depth, COLS), bf16),
                pltpu.VMEM((16 * pp, *piece), bf16),
                pltpu.VMEM((12 * pp, *piece), bf16),
                pltpu.VMEM((2 * blocks, ROWS, d_local // 2), f32),
                pltpu.VMEM((2 * blocks, ROWS, d_local // 2), f32),
                pltpu.VMEM((tok_rows, d_local), bf16),
                pltpu.VMEM((tp, 1, tok_rows), f32),
                dma((2,)),
                dma((W_SLOTS,)),
                dma,
                dma,
                dma,
                dma,
                dma,
                dma,
                dma((2 * blocks,)),
                dma((2,)),
            ],
            compiler_params=pltpu.CompilerParams(
                collective_id=0, has_side_effects=True, vmem_limit_bytes=52 * 2**20
            ),
            name="project_reduce",
        )(attn_blk, w_blk, resid_blk, gain_blk.reshape(1, d_local))
        return pl.pallas_call(
            functools.partial(norm_kernel, tp * d_local),
            out_shape=[jax.ShapeDtypeStruct((tok_rows, d_local), bf16)] * 2,
            in_specs=[vmem] * 4,
            out_specs=[hbm] * 2,
            scratch_shapes=[
                pltpu.VMEM((tok_rows, d_local), bf16),
                dma((2 * tok_rows // OUT_ROWS,)),
            ],
            compiler_params=pltpu.CompilerParams(vmem_limit_bytes=16 * 2**20),
            name="norm_write",
        )(*held)

    return jax.shard_map(
        local_step,
        mesh=mesh,
        in_specs=(P("data", "tp"), P("tp", None), P("data", "tp"), P("tp")),
        out_specs=(P("data", "tp"), P("data", "tp")),
        check_vma=False,
    )
```

```python
import functools

import jax
import jax.numpy as jnp
from jax import lax
from jax.experimental import pallas as pl
from jax.experimental.pallas import tpu as pltpu
from jax.sharding import PartitionSpec as P

EPS = 1e-5
CORES = 2
COLS = 256
W_SLOTS = 6
ROWS = 64
OUT_ROWS = 64


def reduce_kernel(
    tp, d_local, a_hbm, w_hbm, r_hbm, g_hbm, hid, hid_bf, sq_sum, gain,
    a, w, part, recv, relay_out, relay_in, res, sq_all,
    a_sem, w_sem, r_sem, g_sem, send_sem, mid_sem, end_sem, rsend_sem, rrecv_sem, q_sem,
):
    chips = tp // CORES
    half = d_local // 2
    pp = half // COLS
    blk = 4 * pp
    tok_rows = a.shape[0]
    blocks = tok_rows // ROWS
    me = lax.axis_index("tp")
    chip, core = me // CORES, me % CORES

    def w_col(g):
        s, i = g % 2, (g % blk) // 2
        b, p, ph = i % 2, i // 2, g // blk
        is0 = (3 - ph) * (2 - ph) * (1 - ph) // 6
        is1 = ph * (3 - ph) * (2 - ph) // 2
        is2 = ph * (3 - ph) * (ph - 1) // 2
        kept = ph // 2
        step = 2 * s - 1
        hop = is0 * 2 + is1 * step + kept * (1 - b) * step
        mine = (kept - is2) * b + is2 * (1 - b)
        to_core = (1 - kept) * b + kept * (mine * core + (1 - mine) * (1 - core))
        in_half = s + is1 * (1 - 2 * s)
        to = ((chip + chips + hop) % chips) * CORES + to_core
        return to * d_local + in_half * half + p * COLS

    def w_copy(g):
        slot = g % W_SLOTS
        cols = pl.ds(pl.multiple_of(w_col(g), COLS), COLS)
        return pltpu.make_async_copy(w_hbm.at[:, cols], w.at[slot], w_sem.at[slot])

    def number(p, b, s):
        return (2 * p + b) * 2 + s

    def piece_copy(g, sem, rows=slice(None)):
        s, b, ph = g % 2, (g // 2) % 2, g // blk
        far = 1 - ph // 2
        direct = far * ph
        to_chip = (chip + chips + far * (2 * s - 1)) % chips
        to_core = direct * b + (far - direct) * (1 - b) + (1 - far) * (1 - core)
        slot = g + far * (core - b) * 2
        return pltpu.make_async_remote_copy(
            src_ref=part.at[g, rows],
            dst_ref=recv.at[slot, rows],
            send_sem=send_sem,
            recv_sem=sem,
            device_id={"tp": to_chip * CORES + to_core},
            device_id_type=pl.DeviceIdType.MESH,
        )

    def wait_for(ref, sem):
        pltpu.make_async_copy(ref, ref, sem).wait()

    def relay_copy(j):
        to_chip = (chip + chips + 2 * (j % 2) - 1) % chips
        return pltpu.make_async_remote_copy(
            src_ref=relay_out.at[j],
            dst_ref=relay_in.at[j],
            send_sem=rsend_sem,
            recv_sem=rrecv_sem.at[j],
            device_id={"tp": to_chip * CORES + 1 - core},
            device_id_type=pl.DeviceIdType.MESH,
        )

    def peers(hops):
        return [((chip + hop) % chips) * CORES + b for hop in hops for b in range(CORES)]

    partner = chip * CORES + 1 - core
    others = sorted(range(1, chips), key=lambda hop: -min(hop, chips - hop))

    def sq_copy(peer):
        return pltpu.make_async_remote_copy(
            src_ref=sq_all.at[me],
            dst_ref=sq_all.at[me],
            send_sem=q_sem.at[0],
            recv_sem=q_sem.at[1],
            device_id={"tp": peer},
            device_id_type=pl.DeviceIdType.MESH,
        )

    top, low = slice(0, tok_rows // 2), slice(tok_rows // 2, tok_rows)
    a_copies = [
        pltpu.make_async_copy(a_hbm.at[rows], a.at[rows], a_sem.at[i])
        for i, rows in enumerate((top, low))
    ]
    r_copy = pltpu.make_async_copy(r_hbm, res, r_sem)
    g_copy = pltpu.make_async_copy(g_hbm, gain, g_sem)
    a_copies[0].start()
    w_copy(0).start()
    w_copy(1).start()
    a_copies[1].start()
    barrier = pltpu.get_barrier_semaphore()
    near = [partner] + peers((1, chips - 1))
    for peer in near:
        pl.semaphore_signal(
            barrier, inc=1, device_id={"tp": peer}, device_id_type=pl.DeviceIdType.MESH
        )
    for g in range(2, W_SLOTS):
        w_copy(g).start()

    def project(g, rows=slice(None)):
        part[g, rows] = jnp.dot(
            a[rows], w[g % W_SLOTS], preferred_element_type=jnp.float32
        ).astype(jnp.bfloat16)

    for i, rows in enumerate((top, low)):
        a_copies[i].wait()
        for g in range(2):
            if i == 0:
                w_copy(g).wait()
            project(g, rows)
            if i == 0 and g == 0:
                pl.semaphore_wait(barrier, len(near))
            piece_copy(g, mid_sem, rows).start()
    for g in range(2):
        w_copy(W_SLOTS + g).start()

    def step(g, carry):
        w_copy(g).wait()
        project(g)
        b, ph = (g // 2) % 2, g // blk
        for_end = ph % 2 + ph // 2 * b

        @pl.when((g < 3 * blk) & (for_end == 0))
        def _():
            piece_copy(g, mid_sem).start()

        @pl.when((g < 3 * blk) & (for_end == 1))
        def _():
            piece_copy(g, end_sem).start()

        @pl.when(g + W_SLOTS < 4 * blk)
        def _():
            w_copy(g + W_SLOTS).start()

        return carry

    lax.fori_loop(2, 4 * blk, step, 0)
    r_copy.start()
    g_copy.start()
    wait_for(recv.at[pl.ds(0, blk + blk // 2)], mid_sem)

    def row_block(rb):
        return pl.ds(pl.multiple_of(rb * ROWS, ROWS), ROWS)

    def relay(j, carry):
        rows, s = row_block(j // 2), j % 2
        for p in range(pp):
            relay_out[j, :, p * COLS : (p + 1) * COLS] = (
                recv[number(p, 0, s), rows].astype(jnp.float32)
                + recv[number(p, 1, s), rows].astype(jnp.float32)
                + recv[2 * blk + number(p, 0, s), rows].astype(jnp.float32)
                + part[3 * blk + number(p, 0, s), rows].astype(jnp.float32)
            )
        relay_copy(j).start()
        return carry

    lax.fori_loop(0, 2 * blocks, relay, 0)
    r_copy.wait()
    wait_for(recv.at[pl.ds(0, blk + blk // 2)], end_sem)

    def gather(i, carry):
        p, s = i // 2, i % 2
        cols = pl.ds(pl.multiple_of(s * half + p * COLS, COLS), COLS)
        direct = [blk + number(p, b, 1 - s) for b in range(CORES)]
        own = number(p, 1, s)
        hid[:, cols] = (
            res[:, cols].astype(jnp.float32)
            + part[3 * blk + own].astype(jnp.float32)
            + recv[2 * blk + own].astype(jnp.float32)
            + recv[direct[0]].astype(jnp.float32)
            + recv[direct[1]].astype(jnp.float32)
        )
        return carry

    lax.fori_loop(0, 2 * pp, gather, 0)

    totals = []
    for rb in range(blocks):
        rows = slice(rb * ROWS, (rb + 1) * ROWS)
        total = jnp.zeros((ROWS, 128), jnp.float32)
        for s in range(2):
            relay_copy(2 * rb + s).wait_recv()
            for c in range(0, half, 128):
                cols = slice(s * half + c, s * half + c + 128)
                h = hid[rows, cols] + relay_in[2 * rb + s, :, c : c + 128]
                hid[rows, cols] = h
                total += h * h
        totals.append(total)
        if len(totals) * ROWS == 128:
            by_lane = jnp.transpose(jnp.concatenate(totals, axis=0))
            sq_all[me, :, (rb + 1) * ROWS - 128 : (rb + 1) * ROWS] = jnp.sum(
                by_lane, axis=0, keepdims=True
            )
            totals = []
    far_first = peers(others)
    for peer in far_first[1::CORES] + [partner] + far_first[::CORES]:
        sq_copy(peer).start()

    def narrow(rb, carry):
        rows = row_block(rb)
        hid_bf[rows] = hid[rows].astype(jnp.bfloat16)
        return carry

    lax.fori_loop(0, blocks, narrow, 0)
    wait_for(part.at[pl.ds(0, 3 * blk)], send_sem)
    wait_for(relay_out, rsend_sem)
    g_copy.wait()
    wait_for(sq_all.at[pl.ds(0, tp - 1)], q_sem.at[1])
    sq_sum[...] = jnp.sum(sq_all[...], axis=0)
    wait_for(sq_all.at[pl.ds(0, tp - 1)], q_sem.at[0])


def norm_kernel(d_model, hid, hid_bf, sq_sum, gain, hid_out, nrm_out, nrm, sem):
    tok_rows, d_local = hid.shape
    hid_copy = pltpu.make_async_copy(hid_bf, hid_out, sem.at[0])
    hid_copy.start()
    scale_row = lax.rsqrt(sq_sum[...] / d_model + EPS)
    scale = jnp.transpose(jnp.broadcast_to(scale_row, (128, tok_rows)))
    copies = [hid_copy]
    for i, row in enumerate(range(0, tok_rows, OUT_ROWS)):
        rows = slice(row, row + OUT_ROWS)
        for c in range(0, d_local, 128):
            cols = slice(c, c + 128)
            nrm[rows, cols] = (hid[rows, cols] * scale[rows] * gain[:, cols]).astype(jnp.bfloat16)
        copies.append(pltpu.make_async_copy(nrm.at[rows], nrm_out.at[rows], sem.at[1 + i]))
        copies[-1].start()
    for copy in copies:
        copy.wait()


def solution(mesh):
    tp = mesh.shape["tp"]

    def local_step(attn_blk, w_blk, resid_blk, gain_blk):
        tok_rows, depth = attn_blk.shape
        d_local = resid_blk.shape[1]
        pp = d_local // 2 // COLS
        blocks = tok_rows // ROWS
        f32, bf16 = jnp.float32, jnp.bfloat16
        piece = (tok_rows, COLS)
        dma = pltpu.SemaphoreType.DMA
        hbm = pl.BlockSpec(memory_space=pl.ANY)
        vmem = pl.BlockSpec(memory_space=pltpu.VMEM)
        held = pl.pallas_call(
            functools.partial(reduce_kernel, tp, d_local),
            out_shape=[
                pltpu.VMEM((tok_rows, d_local), f32),
                pltpu.VMEM((tok_rows, d_local), bf16),
                pltpu.VMEM((1, tok_rows), f32),
                pltpu.VMEM((1, d_local), f32),
            ],
            in_specs=[hbm] * 4,
            out_specs=[vmem] * 4,
            scratch_shapes=[
                pltpu.VMEM((tok_rows, depth), bf16),
                pltpu.VMEM((W_SLOTS, depth, COLS), bf16),
                pltpu.VMEM((16 * pp, *piece), bf16),
                pltpu.VMEM((12 * pp, *piece), bf16),
                pltpu.VMEM((2 * blocks, ROWS, d_local // 2), f32),
                pltpu.VMEM((2 * blocks, ROWS, d_local // 2), f32),
                pltpu.VMEM((tok_rows, d_local), bf16),
                pltpu.VMEM((tp, 1, tok_rows), f32),
                dma((2,)),
                dma((W_SLOTS,)),
                dma,
                dma,
                dma,
                dma,
                dma,
                dma,
                dma((2 * blocks,)),
                dma((2,)),
            ],
            compiler_params=pltpu.CompilerParams(
                collective_id=0, has_side_effects=True, vmem_limit_bytes=52 * 2**20
            ),
            name="project_reduce",
        )(attn_blk, w_blk, resid_blk, gain_blk.reshape(1, d_local))
        return pl.pallas_call(
            functools.partial(norm_kernel, tp * d_local),
            out_shape=[jax.ShapeDtypeStruct((tok_rows, d_local), bf16)] * 2,
            in_specs=[vmem] * 4,
            out_specs=[hbm] * 2,
            scratch_shapes=[
                pltpu.VMEM((tok_rows, d_local), bf16),
                dma((1 + tok_rows // OUT_ROWS,)),
            ],
            compiler_params=pltpu.CompilerParams(vmem_limit_bytes=16 * 2**20),
            name="norm_write",
        )(*held)

    return jax.shard_map(
        local_step,
        mesh=mesh,
        in_specs=(P("data", "tp"), P("tp", None), P("data", "tp"), P("tp")),
        out_specs=(P("data", "tp"), P("data", "tp")),
        check_vma=False,
    )
```

```python
import functools

import jax
import jax.numpy as jnp
from jax import lax
from jax.experimental import pallas as pl
from jax.experimental.pallas import tpu as pltpu
from jax.sharding import PartitionSpec as P

EPS = 1e-5
CORES = 2
COLS = 256
W_SLOTS = 4
ROWS = 64
OUT_ROWS = 128


def reduce_kernel(
    tp, d_local, a_hbm, w_hbm, r_hbm, g_hbm, hid, hid_bf, sq_all, gain,
    a, w, part, recv, relay_out, relay_in, res,
    a_sem, w_sem, send_sem, mid_sem, end_sem, rsend_sem, rrecv_sem, q_sem,
):
    chips = tp // CORES
    half = d_local // 2
    pp = half // COLS
    blk = 4 * pp
    tok_rows = a.shape[0]
    blocks = tok_rows // ROWS
    me = lax.axis_index("tp")
    chip, core = me // CORES, me % CORES

    def w_col(g):
        s, i = g % 2, (g % blk) // 2
        b, p, ph = i % 2, i // 2, g // blk
        is0 = (3 - ph) * (2 - ph) * (1 - ph) // 6
        is1 = ph * (3 - ph) * (2 - ph) // 2
        is2 = ph * (3 - ph) * (ph - 1) // 2
        kept = ph // 2
        step = 2 * s - 1
        hop = is0 * 2 + is1 * step + kept * (1 - b) * step
        mine = (kept - is2) * b + is2 * (1 - b)
        to_core = (1 - kept) * b + kept * (mine * core + (1 - mine) * (1 - core))
        in_half = s + is1 * (1 - 2 * s)
        to = ((chip + chips + hop) % chips) * CORES + to_core
        return to * d_local + in_half * half + p * COLS

    def w_copy(g):
        slot = g % W_SLOTS
        cols = pl.ds(pl.multiple_of(w_col(g), COLS), COLS)
        return pltpu.make_async_copy(w_hbm.at[:, cols], w.at[slot], w_sem.at[slot])

    def number(p, b, s):
        return (2 * p + b) * 2 + s

    def piece_copy(g, sem, rows=slice(None)):
        s, b, ph = g % 2, (g // 2) % 2, g // blk
        far = 1 - ph // 2
        direct = far * ph
        to_chip = (chip + chips + far * (2 * s - 1)) % chips
        to_core = direct * b + (far - direct) * (1 - b) + (1 - far) * (1 - core)
        slot = g + far * (core - b) * 2
        return pltpu.make_async_remote_copy(
            src_ref=part.at[g, rows],
            dst_ref=recv.at[slot, rows],
            send_sem=send_sem,
            recv_sem=sem,
            device_id={"tp": to_chip * CORES + to_core},
            device_id_type=pl.DeviceIdType.MESH,
        )

    def wait_for(ref, sem):
        pltpu.make_async_copy(ref, ref, sem).wait()

    early = 2 * (blocks - 1)

    def relay_copy(j, sem):
        to_chip = (chip + chips + 2 * (j % 2) - 1) % chips
        return pltpu.make_async_remote_copy(
            src_ref=relay_out.at[j],
            dst_ref=relay_in.at[j],
            send_sem=rsend_sem,
            recv_sem=rrecv_sem.at[sem],
            device_id={"tp": to_chip * CORES + 1 - core},
            device_id_type=pl.DeviceIdType.MESH,
        )

    def peers(hops):
        return [((chip + hop) % chips) * CORES + b for hop in hops for b in range(CORES)]

    partner = chip * CORES + 1 - core
    others = sorted(range(1, chips), key=lambda hop: -min(hop, chips - hop))

    def sq_copy(peer):
        return pltpu.make_async_remote_copy(
            src_ref=sq_all.at[me],
            dst_ref=sq_all.at[me],
            send_sem=q_sem.at[0],
            recv_sem=q_sem.at[1],
            device_id={"tp": peer},
            device_id_type=pl.DeviceIdType.MESH,
        )

    top, low = slice(0, tok_rows // 2), slice(tok_rows // 2, tok_rows)
    a_copies = [
        pltpu.make_async_copy(a_hbm.at[rows], a.at[rows], a_sem.at[i])
        for i, rows in enumerate((top, low))
    ]
    r_copy = pltpu.make_async_copy(r_hbm, res, a_sem.at[0])
    g_copy = pltpu.make_async_copy(g_hbm, gain, a_sem.at[1])
    a_copies[0].start()
    w_copy(0).start()
    w_copy(1).start()
    a_copies[1].start()
    barrier = pltpu.get_barrier_semaphore()
    near = peers((1, chips - 1)) + [partner]
    for peer in near:
        pl.semaphore_signal(
            barrier, inc=1, device_id={"tp": peer}, device_id_type=pl.DeviceIdType.MESH
        )
    for g in range(2, W_SLOTS):
        w_copy(g).start()

    def project(g, rows=slice(None)):
        part[g, rows] = jnp.dot(
            a[rows], w[g % W_SLOTS], preferred_element_type=jnp.float32
        ).astype(jnp.bfloat16)

    for i, rows in enumerate((top, low)):
        a_copies[i].wait()
        for g in range(2):
            if i == 0:
                w_copy(g).wait()
            project(g, rows)
            if i == 0 and g == 0:
                pl.semaphore_wait(barrier, len(near))
            piece_copy(g, mid_sem, rows).start()
    for g in range(2):
        w_copy(W_SLOTS + g).start()

    def step(g, carry):
        w_copy(g).wait()
        project(g)
        b, ph = (g // 2) % 2, g // blk
        for_end = ph % 2 + ph // 2 * b

        @pl.when((g < 3 * blk) & (for_end == 0))
        def _():
            piece_copy(g, mid_sem).start()

        @pl.when((g < 3 * blk) & (for_end == 1))
        def _():
            piece_copy(g, end_sem).start()

        @pl.when(g + W_SLOTS < 4 * blk)
        def _():
            w_copy(g + W_SLOTS).start()

        return carry

    lax.fori_loop(2, 4 * blk, step, 0)
    r_copy.start()
    g_copy.start()
    wait_for(recv.at[pl.ds(0, blk + blk // 2)], mid_sem)

    def row_block(rb):
        return pl.ds(pl.multiple_of(rb * ROWS, ROWS), ROWS)

    def relay(j, sem):
        rows, s = row_block(j // 2), j % 2
        for p in range(pp):
            relay_out[j, :, p * COLS : (p + 1) * COLS] = (
                recv[number(p, 0, s), rows].astype(jnp.float32)
                + recv[number(p, 1, s), rows].astype(jnp.float32)
                + recv[2 * blk + number(p, 0, s), rows].astype(jnp.float32)
                + part[3 * blk + number(p, 0, s), rows].astype(jnp.float32)
            )
        relay_copy(j, sem).start()

    def relay_early(j, carry):
        relay(j, 0)
        return carry

    lax.fori_loop(0, early, relay_early, 0)
    for s in range(2):
        relay(early + s, 1 + s)
    r_copy.wait()
    wait_for(recv.at[pl.ds(0, blk + blk // 2)], end_sem)

    def gather(i, carry):
        p, s = i // 2, i % 2
        cols = pl.ds(pl.multiple_of(s * half + p * COLS, COLS), COLS)
        direct = [blk + number(p, b, 1 - s) for b in range(CORES)]
        own = number(p, 1, s)
        hid[:, cols] = (
            res[:, cols].astype(jnp.float32)
            + part[3 * blk + own].astype(jnp.float32)
            + recv[2 * blk + own].astype(jnp.float32)
            + recv[direct[0]].astype(jnp.float32)
            + recv[direct[1]].astype(jnp.float32)
        )
        return carry

    lax.fori_loop(0, 2 * pp, gather, 0)

    totals = []
    wait_for(relay_in.at[pl.ds(0, early)], rrecv_sem.at[0])
    for rb in range(blocks):
        rows = slice(rb * ROWS, (rb + 1) * ROWS)
        total = jnp.zeros((ROWS, 128), jnp.float32)
        for s in range(2):
            if rb == blocks - 1:
                relay_copy(early + s, 1 + s).wait_recv()
            for c in range(0, half, 128):
                cols = slice(s * half + c, s * half + c + 128)
                h = hid[rows, cols] + relay_in[2 * rb + s, :, c : c + 128]
                hid[rows, cols] = h
                total += h * h
        totals.append(total)
        if len(totals) * ROWS == 128:
            by_lane = jnp.transpose(jnp.concatenate(totals, axis=0))
            sq_all[me, :, (rb + 1) * ROWS - 128 : (rb + 1) * ROWS] = jnp.sum(
                by_lane, axis=0, keepdims=True
            )
            totals = []
    far_first = peers(others)
    for peer in far_first[1::CORES] + [partner] + far_first[::CORES]:
        sq_copy(peer).start()

    def narrow(rb, carry):
        rows = row_block(rb)
        hid_bf[rows] = hid[rows].astype(jnp.bfloat16)
        return carry

    lax.fori_loop(0, blocks, narrow, 0)
    wait_for(part.at[pl.ds(0, 3 * blk)], send_sem)
    wait_for(relay_out, rsend_sem)
    g_copy.wait()
    wait_for(sq_all.at[pl.ds(0, tp - 1)], q_sem.at[1])
    wait_for(sq_all.at[pl.ds(0, tp - 1)], q_sem.at[0])


def norm_kernel(d_model, hid, hid_bf, sq_all, gain, hid_out, nrm_out, nrm, sem):
    tok_rows, d_local = hid.shape
    hid_copy = pltpu.make_async_copy(hid_bf, hid_out, sem.at[0])
    hid_copy.start()
    scale_row = lax.rsqrt(jnp.sum(sq_all[...], axis=0) / d_model + EPS)
    scale = jnp.transpose(jnp.broadcast_to(scale_row, (128, tok_rows)))
    copies = [hid_copy]
    for i, row in enumerate(range(0, tok_rows, OUT_ROWS)):
        rows = slice(row, row + OUT_ROWS)
        for c in range(0, d_local, 128):
            cols = slice(c, c + 128)
            nrm[rows, cols] = (hid[rows, cols] * scale[rows] * gain[:, cols]).astype(jnp.bfloat16)
        copies.append(pltpu.make_async_copy(nrm.at[rows], nrm_out.at[rows], sem.at[1 + i]))
        copies[-1].start()
    for copy in copies:
        copy.wait()


def solution(mesh):
    tp = mesh.shape["tp"]

    def local_step(attn_blk, w_blk, resid_blk, gain_blk):
        tok_rows, depth = attn_blk.shape
        d_local = resid_blk.shape[1]
        pp = d_local // 2 // COLS
        blocks = tok_rows // ROWS
        f32, bf16 = jnp.float32, jnp.bfloat16
        piece = (tok_rows, COLS)
        dma = pltpu.SemaphoreType.DMA
        hbm = pl.BlockSpec(memory_space=pl.ANY)
        vmem = pl.BlockSpec(memory_space=pltpu.VMEM)
        held = pl.pallas_call(
            functools.partial(reduce_kernel, tp, d_local),
            out_shape=[
                pltpu.VMEM((tok_rows, d_local), f32),
                pltpu.VMEM((tok_rows, d_local), bf16),
                pltpu.VMEM((tp, 1, tok_rows), f32),
                pltpu.VMEM((1, d_local), f32),
            ],
            in_specs=[hbm] * 4,
            out_specs=[vmem] * 4,
            scratch_shapes=[
                pltpu.VMEM((tok_rows, depth), bf16),
                pltpu.VMEM((W_SLOTS, depth, COLS), bf16),
                pltpu.VMEM((16 * pp, *piece), bf16),
                pltpu.VMEM((12 * pp, *piece), bf16),
                pltpu.VMEM((2 * blocks, ROWS, d_local // 2), f32),
                pltpu.VMEM((2 * blocks, ROWS, d_local // 2), f32),
                pltpu.VMEM((tok_rows, d_local), bf16),
                dma((2,)),
                dma((W_SLOTS,)),
                dma,
                dma,
                dma,
                dma,
                dma((3,)),
                dma((2,)),
            ],
            compiler_params=pltpu.CompilerParams(
                collective_id=0, has_side_effects=True, vmem_limit_bytes=52 * 2**20
            ),
            name="project_reduce",
        )(attn_blk, w_blk, resid_blk, gain_blk.reshape(1, d_local))
        return pl.pallas_call(
            functools.partial(norm_kernel, tp * d_local),
            out_shape=[jax.ShapeDtypeStruct((tok_rows, d_local), bf16)] * 2,
            in_specs=[vmem] * 4,
            out_specs=[hbm] * 2,
            scratch_shapes=[
                pltpu.VMEM((tok_rows, d_local), bf16),
                dma((1 + tok_rows // OUT_ROWS,)),
            ],
            compiler_params=pltpu.CompilerParams(vmem_limit_bytes=16 * 2**20),
            name="norm_write",
        )(*held)

    return jax.shard_map(
        local_step,
        mesh=mesh,
        in_specs=(P("data", "tp"), P("tp", None), P("data", "tp"), P("tp")),
        out_specs=(P("data", "tp"), P("data", "tp")),
        check_vma=False,
    )
```

```python
import functools

import jax
import jax.numpy as jnp
from jax import lax
from jax.experimental import pallas as pl
from jax.experimental.pallas import tpu as pltpu
from jax.sharding import PartitionSpec as P

EPS = 1e-5
CORES = 2
COLS = 256
W_SLOTS = 4
ROWS = 64
OUT_ROWS = 128


def reduce_kernel(
    tp, d_local, a_hbm, w_hbm, r_hbm, g_hbm, hid, hid_bf, sq_all, gain,
    a, w, part, recv, relay_out, relay_in, res,
    a_sem, w_sem, send_sem, mid_sem, end_sem, rsend_sem, rrecv_sem, q_sem,
):
    chips = tp // CORES
    half = d_local // 2
    pp = half // COLS
    blk = 4 * pp
    tok_rows = a.shape[0]
    blocks = tok_rows // ROWS
    me = lax.axis_index("tp")
    chip, core = me // CORES, me % CORES

    def w_col(g):
        s, i = g % 2, (g % blk) // 2
        b, p, ph = i % 2, i // 2, g // blk
        is0 = (3 - ph) * (2 - ph) * (1 - ph) // 6
        is1 = ph * (3 - ph) * (2 - ph) // 2
        is2 = ph * (3 - ph) * (ph - 1) // 2
        kept = ph // 2
        step = 2 * s - 1
        hop = is0 * 2 + is1 * step + kept * (1 - b) * step
        mine = (kept - is2) * b + is2 * (1 - b)
        to_core = (1 - kept) * b + kept * (mine * core + (1 - mine) * (1 - core))
        in_half = s + is1 * (1 - 2 * s)
        to = ((chip + chips + hop) % chips) * CORES + to_core
        return to * d_local + in_half * half + p * COLS

    def w_copy(g):
        slot = g % W_SLOTS
        cols = pl.ds(pl.multiple_of(w_col(g), COLS), COLS)
        return pltpu.make_async_copy(w_hbm.at[:, cols], w.at[slot], w_sem.at[slot])

    def number(p, b, s):
        return (2 * p + b) * 2 + s

    def piece_copy(g, sem, rows=slice(None)):
        s, b, ph = g % 2, (g // 2) % 2, g // blk
        far = 1 - ph // 2
        direct = far * ph
        to_chip = (chip + chips + far * (2 * s - 1)) % chips
        to_core = direct * b + (far - direct) * (1 - b) + (1 - far) * (1 - core)
        slot = g + far * (core - b) * 2
        return pltpu.make_async_remote_copy(
            src_ref=part.at[g, rows],
            dst_ref=recv.at[slot, rows],
            send_sem=send_sem,
            recv_sem=sem,
            device_id={"tp": to_chip * CORES + to_core},
            device_id_type=pl.DeviceIdType.MESH,
        )

    def wait_for(ref, sem):
        pltpu.make_async_copy(ref, ref, sem).wait()

    early = 2 * (blocks - 1)

    def relay_copy(j, sem):
        to_chip = (chip + chips + 2 * (j % 2) - 1) % chips
        return pltpu.make_async_remote_copy(
            src_ref=relay_out.at[j],
            dst_ref=relay_in.at[j],
            send_sem=rsend_sem,
            recv_sem=rrecv_sem.at[sem],
            device_id={"tp": to_chip * CORES + 1 - core},
            device_id_type=pl.DeviceIdType.MESH,
        )

    def peers(hops):
        return [((chip + hop) % chips) * CORES + b for hop in hops for b in range(CORES)]

    partner = chip * CORES + 1 - core
    others = sorted(range(1, chips), key=lambda hop: min(hop, chips - hop))

    def sq_copy(peer):
        return pltpu.make_async_remote_copy(
            src_ref=sq_all.at[me],
            dst_ref=sq_all.at[me],
            send_sem=q_sem.at[0],
            recv_sem=q_sem.at[1],
            device_id={"tp": peer},
            device_id_type=pl.DeviceIdType.MESH,
        )

    top, low = slice(0, tok_rows // 2), slice(tok_rows // 2, tok_rows)
    a_copies = [
        pltpu.make_async_copy(a_hbm.at[rows], a.at[rows], a_sem.at[i])
        for i, rows in enumerate((top, low))
    ]
    r_copy = pltpu.make_async_copy(r_hbm, res, a_sem.at[0])
    g_copy = pltpu.make_async_copy(g_hbm, gain, a_sem.at[1])
    a_copies[0].start()
    w_copy(0).start()
    w_copy(1).start()
    a_copies[1].start()
    barrier = pltpu.get_barrier_semaphore()
    near = peers((1, chips - 1)) + [partner]
    for peer in near:
        pl.semaphore_signal(
            barrier, inc=1, device_id={"tp": peer}, device_id_type=pl.DeviceIdType.MESH
        )
    for g in range(2, W_SLOTS):
        w_copy(g).start()

    def project(g, rows=slice(None)):
        part[g, rows] = jnp.dot(
            a[rows], w[g % W_SLOTS], preferred_element_type=jnp.float32
        ).astype(jnp.bfloat16)

    for i, rows in enumerate((top, low)):
        a_copies[i].wait()
        for g in range(2):
            if i == 0:
                w_copy(g).wait()
            project(g, rows)
            if i == 0 and g == 0:
                pl.semaphore_wait(barrier, len(near))
            piece_copy(g, mid_sem, rows).start()
    for g in range(2):
        w_copy(W_SLOTS + g).start()

    def step(g, carry):
        w_copy(g).wait()
        project(g)
        b, ph = (g // 2) % 2, g // blk
        for_end = ph % 2 + ph // 2 * b

        @pl.when((g < 3 * blk) & (for_end == 0))
        def _():
            piece_copy(g, mid_sem).start()

        @pl.when((g < 3 * blk) & (for_end == 1))
        def _():
            piece_copy(g, end_sem).start()

        @pl.when(g + W_SLOTS < 4 * blk)
        def _():
            w_copy(g + W_SLOTS).start()

        return carry

    lax.fori_loop(2, 4 * blk, step, 0)
    r_copy.start()
    g_copy.start()
    wait_for(recv.at[pl.ds(0, blk + blk // 2)], mid_sem)

    def row_block(rb):
        return pl.ds(pl.multiple_of(rb * ROWS, ROWS), ROWS)

    def relay(j, sem):
        rows, s = row_block(j // 2), j % 2
        for p in range(pp):
            relay_out[j, :, p * COLS : (p + 1) * COLS] = (
                recv[number(p, 0, s), rows].astype(jnp.float32)
                + recv[number(p, 1, s), rows].astype(jnp.float32)
                + recv[2 * blk + number(p, 0, s), rows].astype(jnp.float32)
                + part[3 * blk + number(p, 0, s), rows].astype(jnp.float32)
            )
        relay_copy(j, sem).start()

    def relay_early(j, carry):
        relay(j, 0)
        return carry

    lax.fori_loop(0, early, relay_early, 0)
    for s in range(2):
        relay(early + s, 1 + s)
    r_copy.wait()
    wait_for(recv.at[pl.ds(0, blk + blk // 2)], end_sem)

    def gather(i, carry):
        p, s = i // 2, i % 2
        cols = pl.ds(pl.multiple_of(s * half + p * COLS, COLS), COLS)
        direct = [blk + number(p, b, 1 - s) for b in range(CORES)]
        own = number(p, 1, s)
        hid[:, cols] = (
            res[:, cols].astype(jnp.float32)
            + part[3 * blk + own].astype(jnp.float32)
            + recv[2 * blk + own].astype(jnp.float32)
            + recv[direct[0]].astype(jnp.float32)
            + recv[direct[1]].astype(jnp.float32)
        )
        return carry

    lax.fori_loop(0, 2 * pp, gather, 0)

    totals = []
    wait_for(relay_in.at[pl.ds(0, early)], rrecv_sem.at[0])
    for rb in range(blocks):
        rows = slice(rb * ROWS, (rb + 1) * ROWS)
        total = jnp.zeros((ROWS, 128), jnp.float32)
        for s in range(2):
            if rb == blocks - 1:
                relay_copy(early + s, 1 + s).wait_recv()
            for c in range(0, half, 128):
                cols = slice(s * half + c, s * half + c + 128)
                h = hid[rows, cols] + relay_in[2 * rb + s, :, c : c + 128]
                hid[rows, cols] = h
                total += h * h
        totals.append(total)
        if len(totals) * ROWS == 128:
            by_lane = jnp.transpose(jnp.concatenate(totals, axis=0))
            sq_all[me, :, (rb + 1) * ROWS - 128 : (rb + 1) * ROWS] = jnp.sum(
                by_lane, axis=0, keepdims=True
            )
            totals = []
    near_first = peers(others)
    for peer in near_first[1::CORES] + [partner] + near_first[::CORES]:
        sq_copy(peer).start()

    def narrow(rb, carry):
        rows = row_block(rb)
        hid_bf[rows] = hid[rows].astype(jnp.bfloat16)
        return carry

    lax.fori_loop(0, blocks, narrow, 0)
    wait_for(part.at[pl.ds(0, 3 * blk)], send_sem)
    wait_for(relay_out, rsend_sem)
    g_copy.wait()
    wait_for(sq_all.at[pl.ds(0, tp - 1)], q_sem.at[1])
    wait_for(sq_all.at[pl.ds(0, tp - 1)], q_sem.at[0])


def norm_kernel(d_model, hid, hid_bf, sq_all, gain, hid_out, nrm_out, nrm, sem):
    tok_rows, d_local = hid.shape
    hid_copy = pltpu.make_async_copy(hid_bf, hid_out, sem.at[0])
    hid_copy.start()
    scale_row = lax.rsqrt(jnp.sum(sq_all[...], axis=0) / d_model + EPS)
    scale = jnp.transpose(jnp.broadcast_to(scale_row, (128, tok_rows)))
    copies = [hid_copy]
    for i, row in enumerate(range(0, tok_rows, OUT_ROWS)):
        rows = slice(row, row + OUT_ROWS)
        for c in range(0, d_local, 128):
            cols = slice(c, c + 128)
            nrm[rows, cols] = (hid[rows, cols] * scale[rows] * gain[:, cols]).astype(jnp.bfloat16)
        copies.append(pltpu.make_async_copy(nrm.at[rows], nrm_out.at[rows], sem.at[1 + i]))
        copies[-1].start()
    for copy in copies:
        copy.wait()


def solution(mesh):
    tp = mesh.shape["tp"]

    def local_step(attn_blk, w_blk, resid_blk, gain_blk):
        tok_rows, depth = attn_blk.shape
        d_local = resid_blk.shape[1]
        pp = d_local // 2 // COLS
        blocks = tok_rows // ROWS
        f32, bf16 = jnp.float32, jnp.bfloat16
        piece = (tok_rows, COLS)
        dma = pltpu.SemaphoreType.DMA
        hbm = pl.BlockSpec(memory_space=pl.ANY)
        vmem = pl.BlockSpec(memory_space=pltpu.VMEM)
        held = pl.pallas_call(
            functools.partial(reduce_kernel, tp, d_local),
            out_shape=[
                pltpu.VMEM((tok_rows, d_local), f32),
                pltpu.VMEM((tok_rows, d_local), bf16),
                pltpu.VMEM((tp, 1, tok_rows), f32),
                pltpu.VMEM((1, d_local), f32),
            ],
            in_specs=[hbm] * 4,
            out_specs=[vmem] * 4,
            scratch_shapes=[
                pltpu.VMEM((tok_rows, depth), bf16),
                pltpu.VMEM((W_SLOTS, depth, COLS), bf16),
                pltpu.VMEM((16 * pp, *piece), bf16),
                pltpu.VMEM((12 * pp, *piece), bf16),
                pltpu.VMEM((2 * blocks, ROWS, d_local // 2), f32),
                pltpu.VMEM((2 * blocks, ROWS, d_local // 2), f32),
                pltpu.VMEM((tok_rows, d_local), bf16),
                dma((2,)),
                dma((W_SLOTS,)),
                dma,
                dma,
                dma,
                dma,
                dma((3,)),
                dma((2,)),
            ],
            compiler_params=pltpu.CompilerParams(
                collective_id=0, has_side_effects=True, vmem_limit_bytes=52 * 2**20
            ),
            name="project_reduce",
        )(attn_blk, w_blk, resid_blk, gain_blk.reshape(1, d_local))
        return pl.pallas_call(
            functools.partial(norm_kernel, tp * d_local),
            out_shape=[jax.ShapeDtypeStruct((tok_rows, d_local), bf16)] * 2,
            in_specs=[vmem] * 4,
            out_specs=[hbm] * 2,
            scratch_shapes=[
                pltpu.VMEM((tok_rows, d_local), bf16),
                dma((1 + tok_rows // OUT_ROWS,)),
            ],
            compiler_params=pltpu.CompilerParams(vmem_limit_bytes=16 * 2**20),
            name="norm_write",
        )(*held)

    return jax.shard_map(
        local_step,
        mesh=mesh,
        in_specs=(P("data", "tp"), P("tp", None), P("data", "tp"), P("tp")),
        out_specs=(P("data", "tp"), P("data", "tp")),
        check_vma=False,
    )
```

```python
import functools

import jax
import jax.numpy as jnp
from jax import lax
from jax.experimental import pallas as pl
from jax.experimental.pallas import tpu as pltpu
from jax.sharding import PartitionSpec as P

EPS = 1e-5
CORES = 2
COLS = 256
W_SLOTS = 4
ROWS = 64
OUT_ROWS = 128


def reduce_kernel(
    tp, d_local, a_hbm, w_hbm, r_hbm, g_hbm, hid, hid_bf, sq_all, gain,
    a, w, part, recv, relay_out, relay_in, res,
    a_sem, w_sem, send_sem, mid_sem, end_sem, rsend_sem, rrecv_sem, q_sem,
):
    chips = tp // CORES
    half = d_local // 2
    pp = half // COLS
    blk = 4 * pp
    tok_rows = a.shape[0]
    blocks = tok_rows // ROWS
    me = lax.axis_index("tp")
    chip, core = me // CORES, me % CORES

    def w_col(g):
        s, i = g % 2, (g % blk) // 2
        b, p, ph = i % 2, i // 2, g // blk
        is0 = (3 - ph) * (2 - ph) * (1 - ph) // 6
        is1 = ph * (3 - ph) * (2 - ph) // 2
        is2 = ph * (3 - ph) * (ph - 1) // 2
        kept = ph // 2
        step = 2 * s - 1
        hop = is0 * 2 + is1 * step + kept * (1 - b) * step
        mine = (kept - is2) * b + is2 * (1 - b)
        to_core = (1 - kept) * b + kept * (mine * core + (1 - mine) * (1 - core))
        in_half = s + is1 * (1 - 2 * s)
        to = ((chip + chips + hop) % chips) * CORES + to_core
        return to * d_local + in_half * half + p * COLS

    def w_copy(g):
        slot = g % W_SLOTS
        cols = pl.ds(pl.multiple_of(w_col(g), COLS), COLS)
        return pltpu.make_async_copy(w_hbm.at[:, cols], w.at[slot], w_sem.at[slot])

    def number(p, b, s):
        return (2 * p + b) * 2 + s

    def piece_copy(g, sem, rows=slice(None)):
        s, b, ph = g % 2, (g // 2) % 2, g // blk
        far = 1 - ph // 2
        direct = far * ph
        to_chip = (chip + chips + far * (2 * s - 1)) % chips
        to_core = direct * b + (far - direct) * (1 - b) + (1 - far) * (1 - core)
        slot = g + far * (core - b) * 2
        return pltpu.make_async_remote_copy(
            src_ref=part.at[g, rows],
            dst_ref=recv.at[slot, rows],
            send_sem=send_sem,
            recv_sem=sem,
            device_id={"tp": to_chip * CORES + to_core},
            device_id_type=pl.DeviceIdType.MESH,
        )

    def wait_for(ref, sem):
        pltpu.make_async_copy(ref, ref, sem).wait()

    early = 2 * (blocks - 1)

    def relay_copy(j, sem):
        to_chip = (chip + chips + 2 * (j % 2) - 1) % chips
        return pltpu.make_async_remote_copy(
            src_ref=relay_out.at[j],
            dst_ref=relay_in.at[j],
            send_sem=rsend_sem,
            recv_sem=rrecv_sem.at[sem],
            device_id={"tp": to_chip * CORES + 1 - core},
            device_id_type=pl.DeviceIdType.MESH,
        )

    def peers(hops):
        return [((chip + hop) % chips) * CORES + b for hop in hops for b in range(CORES)]

    partner = chip * CORES + 1 - core
    others = sorted(range(1, chips), key=lambda hop: -min(hop, chips - hop))

    def sq_copy(peer):
        return pltpu.make_async_remote_copy(
            src_ref=sq_all.at[me],
            dst_ref=sq_all.at[me],
            send_sem=q_sem.at[0],
            recv_sem=q_sem.at[1],
            device_id={"tp": peer},
            device_id_type=pl.DeviceIdType.MESH,
        )

    top, low = slice(0, tok_rows // 2), slice(tok_rows // 2, tok_rows)
    deep = a.shape[1] // 2
    first = []
    for k, a_half_sem, w_half_sem in ((0, a_sem.at[0], w_sem.at[0]), (deep, rsend_sem, q_sem.at[0])):
        ks, cols = pl.ds(k, deep), pl.ds(pl.multiple_of(w_col(0), COLS), COLS)
        first.append(
            (
                pltpu.make_async_copy(a_hbm.at[top, ks], a.at[top, ks], a_half_sem),
                pltpu.make_async_copy(w_hbm.at[ks, cols], w.at[0, ks], w_half_sem),
            )
        )
    a_low = pltpu.make_async_copy(a_hbm.at[low], a.at[low], a_sem.at[1])
    r_copy = pltpu.make_async_copy(r_hbm, res, a_sem.at[0])
    g_copy = pltpu.make_async_copy(g_hbm, gain, a_sem.at[1])
    for copies in first:
        for copy in copies:
            copy.start()
    w_copy(1).start()
    a_low.start()
    barrier = pltpu.get_barrier_semaphore()
    near = peers((1, chips - 1)) + [partner]
    for peer in near:
        pl.semaphore_signal(
            barrier, inc=1, device_id={"tp": peer}, device_id_type=pl.DeviceIdType.MESH
        )
    for g in range(2, W_SLOTS):
        w_copy(g).start()

    def project(g, rows=slice(None)):
        part[g, rows] = jnp.dot(
            a[rows], w[g % W_SLOTS], preferred_element_type=jnp.float32
        ).astype(jnp.bfloat16)

    total = jnp.zeros((tok_rows // 2, COLS), jnp.float32)
    for copies, ks in zip(first, (slice(0, deep), slice(deep, 2 * deep))):
        for copy in copies:
            copy.wait()
        total += jnp.dot(a[top, ks], w[0, ks], preferred_element_type=jnp.float32)
    part[0, top] = total.astype(jnp.bfloat16)
    pl.semaphore_wait(barrier, len(near))
    piece_copy(0, mid_sem, top).start()
    w_copy(1).wait()
    project(1, top)
    piece_copy(1, mid_sem, top).start()
    a_low.wait()
    for g in range(2):
        project(g, low)
        piece_copy(g, mid_sem, low).start()
    for g in range(2):
        w_copy(W_SLOTS + g).start()

    def step(g, carry):
        w_copy(g).wait()
        project(g)
        b, ph = (g // 2) % 2, g // blk
        for_end = ph % 2 + ph // 2 * b

        @pl.when((g < 3 * blk) & (for_end == 0))
        def _():
            piece_copy(g, mid_sem).start()

        @pl.when((g < 3 * blk) & (for_end == 1))
        def _():
            piece_copy(g, end_sem).start()

        @pl.when(g + W_SLOTS < 4 * blk)
        def _():
            w_copy(g + W_SLOTS).start()

        return carry

    lax.fori_loop(2, 4 * blk, step, 0)
    r_copy.start()
    g_copy.start()
    wait_for(recv.at[pl.ds(0, blk + blk // 2)], mid_sem)

    def row_block(rb):
        return pl.ds(pl.multiple_of(rb * ROWS, ROWS), ROWS)

    def relay(j, sem):
        rows, s = row_block(j // 2), j % 2
        for p in range(pp):
            relay_out[j, :, p * COLS : (p + 1) * COLS] = (
                recv[number(p, 0, s), rows].astype(jnp.float32)
                + recv[number(p, 1, s), rows].astype(jnp.float32)
                + recv[2 * blk + number(p, 0, s), rows].astype(jnp.float32)
                + part[3 * blk + number(p, 0, s), rows].astype(jnp.float32)
            )
        relay_copy(j, sem).start()

    def relay_early(j, carry):
        relay(j, 0)
        return carry

    lax.fori_loop(0, early, relay_early, 0)
    for s in range(2):
        relay(early + s, 1 + s)
    r_copy.wait()
    wait_for(recv.at[pl.ds(0, blk + blk // 2)], end_sem)

    def gather(i, carry):
        p, s = i // 2, i % 2
        cols = pl.ds(pl.multiple_of(s * half + p * COLS, COLS), COLS)
        direct = [blk + number(p, b, 1 - s) for b in range(CORES)]
        own = number(p, 1, s)
        hid[:, cols] = (
            res[:, cols].astype(jnp.float32)
            + part[3 * blk + own].astype(jnp.float32)
            + recv[2 * blk + own].astype(jnp.float32)
            + recv[direct[0]].astype(jnp.float32)
            + recv[direct[1]].astype(jnp.float32)
        )
        return carry

    lax.fori_loop(0, 2 * pp, gather, 0)

    totals = []
    wait_for(relay_in.at[pl.ds(0, early)], rrecv_sem.at[0])
    for rb in range(blocks):
        rows = slice(rb * ROWS, (rb + 1) * ROWS)
        total = jnp.zeros((ROWS, 128), jnp.float32)
        for s in range(2):
            if rb == blocks - 1:
                relay_copy(early + s, 1 + s).wait_recv()
            for c in range(0, half, 128):
                cols = slice(s * half + c, s * half + c + 128)
                h = hid[rows, cols] + relay_in[2 * rb + s, :, c : c + 128]
                hid[rows, cols] = h
                total += h * h
        totals.append(total)
        if len(totals) * ROWS == 128:
            by_lane = jnp.transpose(jnp.concatenate(totals, axis=0))
            sq_all[me, :, (rb + 1) * ROWS - 128 : (rb + 1) * ROWS] = jnp.sum(
                by_lane, axis=0, keepdims=True
            )
            totals = []
    far_first = peers(others)
    for peer in far_first[1::CORES] + [partner] + far_first[::CORES]:
        sq_copy(peer).start()

    def narrow(rb, carry):
        rows = row_block(rb)
        hid_bf[rows] = hid[rows].astype(jnp.bfloat16)
        return carry

    lax.fori_loop(0, blocks, narrow, 0)
    wait_for(part.at[pl.ds(0, 3 * blk)], send_sem)
    wait_for(relay_out, rsend_sem)
    g_copy.wait()
    wait_for(sq_all.at[pl.ds(0, tp - 1)], q_sem.at[1])
    wait_for(sq_all.at[pl.ds(0, tp - 1)], q_sem.at[0])


def norm_kernel(d_model, hid, hid_bf, sq_all, gain, hid_out, nrm_out, nrm, sem):
    tok_rows, d_local = hid.shape
    hid_copy = pltpu.make_async_copy(hid_bf, hid_out, sem.at[0])
    hid_copy.start()
    scale_row = lax.rsqrt(jnp.sum(sq_all[...], axis=0) / d_model + EPS)
    scale = jnp.transpose(jnp.broadcast_to(scale_row, (128, tok_rows)))
    copies = [hid_copy]
    for i, row in enumerate(range(0, tok_rows, OUT_ROWS)):
        rows = slice(row, row + OUT_ROWS)
        for c in range(0, d_local, 128):
            cols = slice(c, c + 128)
            nrm[rows, cols] = (hid[rows, cols] * scale[rows] * gain[:, cols]).astype(jnp.bfloat16)
        copies.append(pltpu.make_async_copy(nrm.at[rows], nrm_out.at[rows], sem.at[1 + i]))
        copies[-1].start()
    for copy in copies:
        copy.wait()


def solution(mesh):
    tp = mesh.shape["tp"]

    def local_step(attn_blk, w_blk, resid_blk, gain_blk):
        tok_rows, depth = attn_blk.shape
        d_local = resid_blk.shape[1]
        pp = d_local // 2 // COLS
        blocks = tok_rows // ROWS
        f32, bf16 = jnp.float32, jnp.bfloat16
        piece = (tok_rows, COLS)
        dma = pltpu.SemaphoreType.DMA
        hbm = pl.BlockSpec(memory_space=pl.ANY)
        vmem = pl.BlockSpec(memory_space=pltpu.VMEM)
        held = pl.pallas_call(
            functools.partial(reduce_kernel, tp, d_local),
            out_shape=[
                pltpu.VMEM((tok_rows, d_local), f32),
                pltpu.VMEM((tok_rows, d_local), bf16),
                pltpu.VMEM((tp, 1, tok_rows), f32),
                pltpu.VMEM((1, d_local), f32),
            ],
            in_specs=[hbm] * 4,
            out_specs=[vmem] * 4,
            scratch_shapes=[
                pltpu.VMEM((tok_rows, depth), bf16),
                pltpu.VMEM((W_SLOTS, depth, COLS), bf16),
                pltpu.VMEM((16 * pp, *piece), bf16),
                pltpu.VMEM((12 * pp, *piece), bf16),
                pltpu.VMEM((2 * blocks, ROWS, d_local // 2), f32),
                pltpu.VMEM((2 * blocks, ROWS, d_local // 2), f32),
                pltpu.VMEM((tok_rows, d_local), bf16),
                dma((2,)),
                dma((W_SLOTS,)),
                dma,
                dma,
                dma,
                dma,
                dma((3,)),
                dma((2,)),
            ],
            compiler_params=pltpu.CompilerParams(
                collective_id=0, has_side_effects=True, vmem_limit_bytes=52 * 2**20
            ),
            name="project_reduce",
        )(attn_blk, w_blk, resid_blk, gain_blk.reshape(1, d_local))
        return pl.pallas_call(
            functools.partial(norm_kernel, tp * d_local),
            out_shape=[jax.ShapeDtypeStruct((tok_rows, d_local), bf16)] * 2,
            in_specs=[vmem] * 4,
            out_specs=[hbm] * 2,
            scratch_shapes=[
                pltpu.VMEM((tok_rows, d_local), bf16),
                dma((1 + tok_rows // OUT_ROWS,)),
            ],
            compiler_params=pltpu.CompilerParams(vmem_limit_bytes=16 * 2**20),
            name="norm_write",
        )(*held)

    return jax.shard_map(
        local_step,
        mesh=mesh,
        in_specs=(P("data", "tp"), P("tp", None), P("data", "tp"), P("tp")),
        out_specs=(P("data", "tp"), P("data", "tp")),
        check_vma=False,
    )
```

```python
import functools

import jax
import jax.numpy as jnp
from jax import lax
from jax.experimental import pallas as pl
from jax.experimental.pallas import tpu as pltpu
from jax.sharding import PartitionSpec as P

EPS = 1e-5
CORES = 2
COLS = 256
W_SLOTS = 4
ROWS = 32
OUT_ROWS = 128


def reduce_kernel(
    tp, d_local, a_hbm, w_hbm, r_hbm, g_hbm, hid, hid_bf, sq_all, gain,
    a, w, part, recv, relay_out, relay_in, res,
    a_sem, w_sem, send_sem, mid_sem, end_sem, rsend_sem, rrecv_sem, q_sem,
):
    chips = tp // CORES
    half = d_local // 2
    pp = half // COLS
    blk = 4 * pp
    tok_rows = a.shape[0]
    blocks = tok_rows // ROWS
    me = lax.axis_index("tp")
    chip, core = me // CORES, me % CORES

    def w_col(g):
        s, i = g % 2, (g % blk) // 2
        b, p, ph = i % 2, i // 2, g // blk
        is0 = (3 - ph) * (2 - ph) * (1 - ph) // 6
        is1 = ph * (3 - ph) * (2 - ph) // 2
        is2 = ph * (3 - ph) * (ph - 1) // 2
        kept = ph // 2
        step = 2 * s - 1
        hop = is0 * 2 + is1 * step + kept * (1 - b) * step
        mine = (kept - is2) * b + is2 * (1 - b)
        to_core = (1 - kept) * b + kept * (mine * core + (1 - mine) * (1 - core))
        in_half = s + is1 * (1 - 2 * s)
        to = ((chip + chips + hop) % chips) * CORES + to_core
        return to * d_local + in_half * half + p * COLS

    def w_copy(g):
        slot = g % W_SLOTS
        cols = pl.ds(pl.multiple_of(w_col(g), COLS), COLS)
        return pltpu.make_async_copy(w_hbm.at[:, cols], w.at[slot], w_sem.at[slot])

    def number(p, b, s):
        return (2 * p + b) * 2 + s

    def piece_copy(g, sem, rows=slice(None)):
        s, b, ph = g % 2, (g // 2) % 2, g // blk
        far = 1 - ph // 2
        direct = far * ph
        to_chip = (chip + chips + far * (2 * s - 1)) % chips
        to_core = direct * b + (far - direct) * (1 - b) + (1 - far) * (1 - core)
        slot = g + far * (core - b) * 2
        return pltpu.make_async_remote_copy(
            src_ref=part.at[g, rows],
            dst_ref=recv.at[slot, rows],
            send_sem=send_sem,
            recv_sem=sem,
            device_id={"tp": to_chip * CORES + to_core},
            device_id_type=pl.DeviceIdType.MESH,
        )

    def wait_for(ref, sem):
        pltpu.make_async_copy(ref, ref, sem).wait()

    early = 2 * (blocks - 1)

    def relay_copy(j, sem):
        to_chip = (chip + chips + 2 * (j % 2) - 1) % chips
        return pltpu.make_async_remote_copy(
            src_ref=relay_out.at[j],
            dst_ref=relay_in.at[j],
            send_sem=rsend_sem,
            recv_sem=rrecv_sem.at[sem],
            device_id={"tp": to_chip * CORES + 1 - core},
            device_id_type=pl.DeviceIdType.MESH,
        )

    def peers(hops):
        return [((chip + hop) % chips) * CORES + b for hop in hops for b in range(CORES)]

    partner = chip * CORES + 1 - core
    others = sorted(range(1, chips), key=lambda hop: -min(hop, chips - hop))

    def sq_copy(peer):
        return pltpu.make_async_remote_copy(
            src_ref=sq_all.at[me],
            dst_ref=sq_all.at[me],
            send_sem=q_sem.at[0],
            recv_sem=q_sem.at[1],
            device_id={"tp": peer},
            device_id_type=pl.DeviceIdType.MESH,
        )

    top, low = slice(0, tok_rows // 2), slice(tok_rows // 2, tok_rows)
    deep = a.shape[1] // 2
    first = []
    for k, a_half_sem, w_half_sem in ((0, a_sem.at[0], w_sem.at[0]), (deep, rsend_sem, q_sem.at[0])):
        ks, cols = pl.ds(k, deep), pl.ds(pl.multiple_of(w_col(0), COLS), COLS)
        first.append(
            (
                pltpu.make_async_copy(a_hbm.at[top, ks], a.at[top, ks], a_half_sem),
                pltpu.make_async_copy(w_hbm.at[ks, cols], w.at[0, ks], w_half_sem),
            )
        )
    a_low = pltpu.make_async_copy(a_hbm.at[low], a.at[low], a_sem.at[1])
    r_copy = pltpu.make_async_copy(r_hbm, res, a_sem.at[0])
    g_copy = pltpu.make_async_copy(g_hbm, gain, a_sem.at[1])
    for copies in first:
        for copy in copies:
            copy.start()
    w_copy(1).start()
    a_low.start()
    barrier = pltpu.get_barrier_semaphore()
    near = peers((1, chips - 1)) + [partner]
    for peer in near:
        pl.semaphore_signal(
            barrier, inc=1, device_id={"tp": peer}, device_id_type=pl.DeviceIdType.MESH
        )
    for g in range(2, W_SLOTS):
        w_copy(g).start()

    def project(g, rows=slice(None)):
        part[g, rows] = jnp.dot(
            a[rows], w[g % W_SLOTS], preferred_element_type=jnp.float32
        ).astype(jnp.bfloat16)

    total = jnp.zeros((tok_rows // 2, COLS), jnp.float32)
    for copies, ks in zip(first, (slice(0, deep), slice(deep, 2 * deep))):
        for copy in copies:
            copy.wait()
        total += jnp.dot(a[top, ks], w[0, ks], preferred_element_type=jnp.float32)
    part[0, top] = total.astype(jnp.bfloat16)
    pl.semaphore_wait(barrier, len(near))
    piece_copy(0, mid_sem, top).start()
    w_copy(1).wait()
    project(1, top)
    piece_copy(1, mid_sem, top).start()
    a_low.wait()
    for g in range(2):
        project(g, low)
        piece_copy(g, mid_sem, low).start()
    for g in range(2):
        w_copy(W_SLOTS + g).start()

    def step(g, carry):
        w_copy(g).wait()
        project(g)
        b, ph = (g // 2) % 2, g // blk
        for_end = ph % 2 + ph // 2 * b

        @pl.when((g < 3 * blk) & (for_end == 0))
        def _():
            piece_copy(g, mid_sem).start()

        @pl.when((g < 3 * blk) & (for_end == 1))
        def _():
            piece_copy(g, end_sem).start()

        @pl.when(g + W_SLOTS < 4 * blk)
        def _():
            w_copy(g + W_SLOTS).start()

        return carry

    lax.fori_loop(2, 4 * blk, step, 0)
    r_copy.start()
    g_copy.start()
    wait_for(recv.at[pl.ds(0, blk + blk // 2)], mid_sem)

    def row_block(rb):
        return pl.ds(pl.multiple_of(rb * ROWS, ROWS), ROWS)

    def relay(j, sem):
        rows, s = row_block(j // 2), j % 2
        for p in range(pp):
            relay_out[j, :, p * COLS : (p + 1) * COLS] = (
                recv[number(p, 0, s), rows].astype(jnp.float32)
                + recv[number(p, 1, s), rows].astype(jnp.float32)
                + recv[2 * blk + number(p, 0, s), rows].astype(jnp.float32)
                + part[3 * blk + number(p, 0, s), rows].astype(jnp.float32)
            )
        relay_copy(j, sem).start()

    def relay_early(j, carry):
        relay(j, 0)
        return carry

    lax.fori_loop(0, early, relay_early, 0)
    for s in range(2):
        relay(early + s, 1 + s)
    r_copy.wait()
    wait_for(recv.at[pl.ds(0, blk + blk // 2)], end_sem)

    def gather(i, carry):
        p, s = i // 2, i % 2
        cols = pl.ds(pl.multiple_of(s * half + p * COLS, COLS), COLS)
        direct = [blk + number(p, b, 1 - s) for b in range(CORES)]
        own = number(p, 1, s)
        hid[:, cols] = (
            res[:, cols].astype(jnp.float32)
            + part[3 * blk + own].astype(jnp.float32)
            + recv[2 * blk + own].astype(jnp.float32)
            + recv[direct[0]].astype(jnp.float32)
            + recv[direct[1]].astype(jnp.float32)
        )
        return carry

    lax.fori_loop(0, 2 * pp, gather, 0)

    totals = []
    wait_for(relay_in.at[pl.ds(0, early)], rrecv_sem.at[0])
    for rb in range(blocks):
        rows = slice(rb * ROWS, (rb + 1) * ROWS)
        total = jnp.zeros((ROWS, 128), jnp.float32)
        for s in range(2):
            if rb == blocks - 1:
                relay_copy(early + s, 1 + s).wait_recv()
            for c in range(0, half, 128):
                cols = slice(s * half + c, s * half + c + 128)
                h = hid[rows, cols] + relay_in[2 * rb + s, :, c : c + 128]
                hid[rows, cols] = h
                total += h * h
        totals.append(total)
        if len(totals) * ROWS == 128:
            by_lane = jnp.transpose(jnp.concatenate(totals, axis=0))
            sq_all[me, :, (rb + 1) * ROWS - 128 : (rb + 1) * ROWS] = jnp.sum(
                by_lane, axis=0, keepdims=True
            )
            totals = []
    far_first = peers(others)
    for peer in far_first[1::CORES] + [partner] + far_first[::CORES]:
        sq_copy(peer).start()

    def narrow(rb, carry):
        rows = row_block(rb)
        hid_bf[rows] = hid[rows].astype(jnp.bfloat16)
        return carry

    lax.fori_loop(0, blocks, narrow, 0)
    wait_for(part.at[pl.ds(0, 3 * blk)], send_sem)
    wait_for(relay_out, rsend_sem)
    g_copy.wait()
    wait_for(sq_all.at[pl.ds(0, tp - 1)], q_sem.at[1])
    wait_for(sq_all.at[pl.ds(0, tp - 1)], q_sem.at[0])


def norm_kernel(d_model, hid, hid_bf, sq_all, gain, hid_out, nrm_out, nrm, sem):
    tok_rows, d_local = hid.shape
    hid_copy = pltpu.make_async_copy(hid_bf, hid_out, sem.at[0])
    hid_copy.start()
    scale_row = lax.rsqrt(jnp.sum(sq_all[...], axis=0) / d_model + EPS)
    scale = jnp.transpose(jnp.broadcast_to(scale_row, (128, tok_rows)))
    copies = [hid_copy]
    for i, row in enumerate(range(0, tok_rows, OUT_ROWS)):
        rows = slice(row, row + OUT_ROWS)
        for c in range(0, d_local, 128):
            cols = slice(c, c + 128)
            nrm[rows, cols] = (hid[rows, cols] * scale[rows] * gain[:, cols]).astype(jnp.bfloat16)
        copies.append(pltpu.make_async_copy(nrm.at[rows], nrm_out.at[rows], sem.at[1 + i]))
        copies[-1].start()
    for copy in copies:
        copy.wait()


def solution(mesh):
    tp = mesh.shape["tp"]

    def local_step(attn_blk, w_blk, resid_blk, gain_blk):
        tok_rows, depth = attn_blk.shape
        d_local = resid_blk.shape[1]
        pp = d_local // 2 // COLS
        blocks = tok_rows // ROWS
        f32, bf16 = jnp.float32, jnp.bfloat16
        piece = (tok_rows, COLS)
        dma = pltpu.SemaphoreType.DMA
        hbm = pl.BlockSpec(memory_space=pl.ANY)
        vmem = pl.BlockSpec(memory_space=pltpu.VMEM)
        held = pl.pallas_call(
            functools.partial(reduce_kernel, tp, d_local),
            out_shape=[
                pltpu.VMEM((tok_rows, d_local), f32),
                pltpu.VMEM((tok_rows, d_local), bf16),
                pltpu.VMEM((tp, 1, tok_rows), f32),
                pltpu.VMEM((1, d_local), f32),
            ],
            in_specs=[hbm] * 4,
            out_specs=[vmem] * 4,
            scratch_shapes=[
                pltpu.VMEM((tok_rows, depth), bf16),
                pltpu.VMEM((W_SLOTS, depth, COLS), bf16),
                pltpu.VMEM((16 * pp, *piece), bf16),
                pltpu.VMEM((12 * pp, *piece), bf16),
                pltpu.VMEM((2 * blocks, ROWS, d_local // 2), f32),
                pltpu.VMEM((2 * blocks, ROWS, d_local // 2), f32),
                pltpu.VMEM((tok_rows, d_local), bf16),
                dma((2,)),
                dma((W_SLOTS,)),
                dma,
                dma,
                dma,
                dma,
                dma((3,)),
                dma((2,)),
            ],
            compiler_params=pltpu.CompilerParams(
                collective_id=0, has_side_effects=True, vmem_limit_bytes=52 * 2**20
            ),
            name="project_reduce",
        )(attn_blk, w_blk, resid_blk, gain_blk.reshape(1, d_local))
        return pl.pallas_call(
            functools.partial(norm_kernel, tp * d_local),
            out_shape=[jax.ShapeDtypeStruct((tok_rows, d_local), bf16)] * 2,
            in_specs=[vmem] * 4,
            out_specs=[hbm] * 2,
            scratch_shapes=[
                pltpu.VMEM((tok_rows, d_local), bf16),
                dma((1 + tok_rows // OUT_ROWS,)),
            ],
            compiler_params=pltpu.CompilerParams(vmem_limit_bytes=16 * 2**20),
            name="norm_write",
        )(*held)

    return jax.shard_map(
        local_step,
        mesh=mesh,
        in_specs=(P("data", "tp"), P("tp", None), P("data", "tp"), P("tp")),
        out_specs=(P("data", "tp"), P("data", "tp")),
        check_vma=False,
    )
```
